256 devices in a mesh: expert: 64 (over z, x, core), replica: 4 (over y).
Axes of the slice: x: 4, y: 4, z: 8, core: 2. Of those that a mesh axis runs over, the one named last changes fastest.
Arguments:
- tokens: bfloat16 [32768, 2048], P(('expert', 'replica')), may hold values from -24 to 24
- cotangent: bfloat16 [32768, 2048], P(('expert', 'replica')), may hold values from -6 to 6
- route_weights: float32 [32768, 8], P(('expert', 'replica')), may hold values from 0.02 to 0.4
- expert_ids: int32 [32768, 8], P(('expert', 'replica')), may hold values from 0 to 127, as said below
- slot_ids: int32 [32768, 8], P(('expert', 'replica')), may hold values from 0 to 7, as said below
- kept_mask: int32 [32768, 8], P(('expert', 'replica')), may hold values from 0 to 1, as said below
- gate_weight: bfloat16 [128, 2048, 384], P('expert'), may hold values from -0.125 to 0.125
- up_weight: bfloat16 [128, 2048, 384], P('expert'), may hold values from -0.125 to 0.125
- down_weight: bfloat16 [128, 384, 2048], P('expert'), may hold values from -0.3125 to 0.3125
- projector_basis: float32 [2048, 256], P('expert'), may hold values from -6 to 6
Outputs:
- token_grads: bfloat16 [32768, 2048], P(('expert', 'replica'))
- projected_grads: float32 [128, 3, 384, 256], P('expert')
- new_basis: float32 [2048, 256], P('expert')
The draws below stay inside these ranges and needn't reach their ends.
Inputs may be any that keep to these rules, and one draw needn't show every extreme that they name: `expert_ids`: each row names 8 different experts. `slot_ids`: within one device's rows, the kept routes to one expert take slots 0, 1, 2, ... in the order of rows and then of the position in the row; a dropped route has slot 0; in every draw some expert receives 8 kept routes from every device's rows. `kept_mask`: a route is dropped exactly when 8 earlier routes of the same device's rows go to the same expert.
All inputs are finite; a program needn't handle non-finite values.
Results may differ from the reference program's by a relative error of at most 0.019.
Values may be sent and summed in bfloat16 or wider, within the bound.
No kernel may reach another device: no remote copies, remote signals or barrier semaphores. Data moves between devices by JAX's collectives and lax.ppermute only.
A program may use at most 128 MiB of HBM per device.

```python
import math
import jax
import jax.numpy as jnp
from jax import lax

D = 2048
TOP = 8
FF = 384
RANK = 256
TOK_DEV = 128
SPECIALIST_TOTAL = 128
CAP = 8
TOKENS = 32768
N_EXPERT = 64
N_REPLICA = 4


def routing_tables(key):
    key = jax.random.fold_in(key, 4242)
    noise_key, level_key, favored_key, coin_key = jax.random.split(key, 4)
    blocks = TOKENS // TOK_DEV
    stochastic_perturbation = jax.random.randint(noise_key, (TOKENS, SPECIALIST_TOTAL), 0, 4096)
    perturbation_magnitude = jax.random.randint(level_key, (SPECIALIST_TOTAL,), 0, 4) * 1024
    favorite_specialist = jax.random.randint(favored_key, (), 0, SPECIALIST_TOTAL)
    coin = jax.random.randint(coin_key, (TOKENS,), 0, 2)
    position = jnp.arange(TOKENS) % TOK_DEV
    chosen_specialists = jnp.logical_or(coin > 0, position < CAP)
    entry_positions = jnp.arange(SPECIALIST_TOTAL)[None, :]
    logit_increment = jnp.where(jnp.logical_and(chosen_specialists[:, None], entry_positions == favorite_specialist), 65536, 0)
    gating_logit = (stochastic_perturbation + perturbation_magnitude[None, :] + logit_increment) * SPECIALIST_TOTAL + entry_positions
    picked = lax.top_k(gating_logit, TOP)[1].astype(jnp.int32)
    onehot = (picked[:, :, None] == jnp.arange(SPECIALIST_TOTAL)[None, None, :]).astype(jnp.int32)
    onehot = onehot.reshape(blocks, TOK_DEV * TOP, SPECIALIST_TOTAL)
    running = jnp.cumsum(onehot, axis=1)
    ranking = (jnp.sum(onehot * running, axis=-1) - 1).reshape(TOKENS, TOP)
    kept = (ranking < CAP).astype(jnp.int32)
    slots = jnp.where(kept > 0, ranking, 0).astype(jnp.int32)
    return (picked, slots, kept)


def draw_expert_ids(key, part):
    return routing_tables(key)[0]


def draw_slot_ids(key, part):
    return routing_tables(key)[1]


def draw_kept_mask(key, part):
    return routing_tables(key)[2]


def raised(result, own_key, source, target, parts, factor):
    owner, partner = [(jnp.arange(result.shape[dim]) // (result.shape[dim] // parts)).reshape([-1 if axis == dim else 1 for axis in range(result.ndim)]) for dim in (source, target)]
    chosen = jax.random.permutation(own_key, parts)[partner]
    strong = (owner == chosen) | (owner == (partner + parts // 2) % parts)
    return jnp.where(strong, factor * result, result)


def levels(rng, dims, pieces, least, top_value):
    loudness = 1.0
    for dim, parts in pieces:
        steps = jax.random.uniform(jax.random.fold_in(jax.random.fold_in(rng, 6), dim), (parts,), jnp.float32, least / len(pieces), top_value / len(pieces))
        loudness = loudness * jnp.repeat(jnp.exp(steps), dims[dim] // parts).reshape((-1,) + (1,) * (len(dims) - 1 - dim))
    return loudness


def normal_values(own_key, dims, spread, bound, pieces=(), kind=jnp.bfloat16):
    result = spread * jax.random.normal(own_key, dims, jnp.float32)
    if pieces:
        result = result * levels(own_key, dims, pieces, -0.22, 0.18)
    return jnp.clip(result, -bound, bound).astype(kind)


def heavy_noise(rng, shape, deviation, bound, pieces, heavy, kind=jnp.bfloat16):
    result = deviation * jax.random.normal(rng, shape, jnp.float32)
    if pieces:
        result = result * levels(rng, shape, pieces, -0.22, 0.18)
    return jnp.clip(raised(result, jax.random.fold_in(rng, 3), *heavy), -bound, bound).astype(kind)


def setup_inputs(seed: int = 0) -> dict:
    keys = jax.random.split(jax.random.key(seed), 11)
    tokens = heavy_noise(keys[0], (TOKENS, D), 1.0, 24.0, ((0, 256),), (0, 1, 256, 6.0))
    cotangent = normal_values(keys[1], (TOKENS, D), 1.0, 6.0, ((0, 256),))
    route_weights = jnp.clip(0.02 + 0.38 * jax.random.uniform(keys[2], (TOKENS, TOP), jnp.float32) ** levels(keys[2], (TOKENS, TOP), ((0, 256),), -0.2, 0.2), 0.02, 0.4)
    expert_ids = draw_expert_ids(jax.random.fold_in(keys[10], 71), 0)
    slot_ids = draw_slot_ids(jax.random.fold_in(keys[10], 71), 0)
    kept_mask = draw_kept_mask(jax.random.fold_in(keys[10], 71), 0)
    gate_weight = normal_values(keys[6], (SPECIALIST_TOTAL, D, FF), D ** -0.5, 0.125, ((0, 64),))
    up_weight = normal_values(keys[7], (SPECIALIST_TOTAL, D, FF), D ** -0.5, 0.125, ((0, 64),))
    down_weight = normal_values(keys[8], (SPECIALIST_TOTAL, FF, D), FF ** -0.5, 0.3125, ((0, 64),))
    projector_basis = normal_values(keys[9], (D, RANK), 1.0, 6.0, ((0, 64),), jnp.float32)
    return {"tokens": tokens, "cotangent": cotangent, "route_weights": route_weights, "expert_ids": expert_ids, "slot_ids": slot_ids, "kept_mask": kept_mask, "gate_weight": gate_weight, "up_weight": up_weight, "down_weight": down_weight, "projector_basis": projector_basis}


def silu_parts(gate):
    sigma = jax.nn.sigmoid(gate)
    return (gate * sigma, sigma * (1.0 + gate * (1.0 - sigma)))

def rounded(value):
    return lax.optimization_barrier(value.astype(jnp.bfloat16)).astype(jnp.float32)

def reference(tokens, cotangent, route_weights, expert_ids, slot_ids, kept_mask, gate_weight, up_weight, down_weight, projector_basis):
    per_expert = N_EXPERT * CAP
    device_of = jnp.arange(TOKENS, dtype=jnp.int32) // TOK_DEV
    source_of = (device_of // N_REPLICA)[:, None]
    replica_of = (device_of % N_REPLICA)[:, None]
    empty_slot = SPECIALIST_TOTAL * N_REPLICA * per_expert
    target = jnp.where(kept_mask > 0, (expert_ids * N_REPLICA + replica_of) * per_expert + source_of * CAP + slot_ids, empty_slot).astype(jnp.int32)
    route_count = TOKENS * TOP
    table = jnp.full((empty_slot,), route_count, jnp.int32).at[target.reshape(-1)].set(jnp.arange(route_count, dtype=jnp.int32), mode='drop')
    table = table.reshape(SPECIALIST_TOTAL, N_REPLICA, per_expert)
    tokens_pad = jnp.concatenate([tokens, jnp.zeros((1, D), tokens.dtype)], 0)
    cotangent_pad = jnp.concatenate([cotangent, jnp.zeros((1, D), cotangent.dtype)], 0)
    weight_pad = jnp.concatenate([route_weights.reshape(-1), jnp.zeros((1,), route_weights.dtype)], 0)
    projector = rounded(projector_basis * (1.0 / math.sqrt(D)))

    def expert_step(power, inputs):
        routes, w_gate, w_up, w_down = inputs
        owner = routes // TOP
        x_rows = tokens_pad[owner].astype(jnp.float32)
        dy_rows = rounded(cotangent_pad[owner].astype(jnp.float32) * weight_pad[routes][..., None])
        gate_full = w_gate.astype(jnp.float32)
        up_full = w_up.astype(jnp.float32)
        gate = jnp.einsum('rpd,df->rpf', x_rows, gate_full)
        upper = jnp.einsum('rpd,df->rpf', x_rows, up_full)
        activated, slope = silu_parts(gate)
        hidden = rounded(activated * upper)
        hidden_grad = jnp.einsum('rpd,fd->rpf', dy_rows, w_down.astype(jnp.float32))
        up_grad = rounded(hidden_grad * activated)
        gate_grad = rounded(hidden_grad * upper * slope)
        row_grads = (jnp.einsum('rpf,df->rpd', gate_grad, gate_full) + jnp.einsum('rpf,df->rpd', up_grad, up_full)).astype(jnp.bfloat16)
        x_proj = rounded(jnp.einsum('rpd,dk->rpk', x_rows, projector))
        dy_proj = rounded(jnp.einsum('rpd,dk->rpk', dy_rows, projector))
        grads = jnp.stack([jnp.einsum('rpf,rpk->fk', gate_grad, x_proj), jnp.einsum('rpf,rpk->fk', up_grad, x_proj), jnp.einsum('rpf,rpk->fk', hidden, dy_proj)], 0)
        grads_low = rounded(grads)
        mixed = rounded(jnp.einsum('rpf,fk->rpk', gate_grad, grads_low[0]) + jnp.einsum('rpf,fk->rpk', up_grad, grads_low[1]))
        down_mix = rounded(jnp.einsum('rpf,fk->rpk', hidden, grads_low[2]))
        power = power + jnp.einsum('rpd,rpk->dk', x_rows, mixed) + jnp.einsum('rpd,rpk->dk', dy_rows, down_mix)
        return (power, (row_grads, grads))
    power, (row_grads, projected_grads) = lax.scan(expert_step, jnp.zeros((D, RANK), jnp.float32), (table, gate_weight, up_weight, down_weight))
    back = jnp.concatenate([row_grads.reshape(empty_slot, D), jnp.zeros((1, D), jnp.bfloat16)], 0)

    def combine(block_targets):
        return lax.optimization_barrier(jnp.sum(back[block_targets].astype(jnp.float32), axis=1)).astype(jnp.bfloat16)
    token_grads = lax.map(combine, target.reshape(TOKENS // TOK_DEV, TOK_DEV, TOP)).reshape(TOKENS, D)
    gram = jnp.dot(power.T.astype(jnp.float32), power.astype(jnp.float32), precision=lax.Precision.HIGHEST, preferred_element_type=jnp.float32)
    lower = jnp.linalg.cholesky(gram)
    new_basis = math.sqrt(D) * jax.scipy.linalg.solve_triangular(lower, power.T, lower=True).T
    return (token_grads, projected_grads, new_basis)
```

```python
import math

import jax
import jax.numpy as jnp
from jax import lax
from jax.experimental import pallas as pl
from jax.experimental.pallas import tpu as pltpu
from jax.sharding import Mesh
from jax.sharding import PartitionSpec as P

Z, X, C, Y = "expert_0", "expert_1", "expert_2", "replica"
EXPERT = (Z, X, C)
EXPERT_REPLICA = (Z, X, C, Y)
PLANE = (X, C)
PAIR = 2
RADIX = 256
DROPPED = 255 * RADIX
SHIFT = float(1 << 17)
SIDE = 128
BLOCK = 64


f32, bf16 = jnp.float32, jnp.bfloat16


def dot(a, b, over=((1,), (0,)), precision=None):
    return lax.dot_general(a, b, (over, ((), ())), precision=precision, preferred_element_type=f32)


def cost(flops, nbytes):
    return pl.CostEstimate(flops=int(flops), bytes_accessed=int(nbytes), transcendentals=0)


def from_everyone(array, axis):
    copies = jnp.broadcast_to(array, (lax.axis_size(axis), *array.shape))
    return lax.all_to_all(copies, axis, split_axis=0, concat_axis=0, tiled=True)


def sent_and_summed(lines, axis):
    devices = lax.axis_size(axis)
    pieces = lines.reshape(devices, -1, lines.shape[-1])
    arrived = lax.all_to_all(pieces, axis, split_axis=0, concat_axis=0, tiled=True)
    return arrived.astype(f32).sum(axis=0).astype(bf16)


def gathered(lines, axis):
    return from_everyone(lines, axis).reshape(-1, lines.shape[-1])


def packed_body(cap, tokens, expert_ids, slot_ids, kept_mask, route_weights, out):
    width = tokens.shape[1]
    target = jnp.where(kept_mask[...] > 0, expert_ids[...] * cap + slot_ids[...], DROPPED)
    weight = route_weights[...]
    first = weight.astype(bf16)
    rest = weight - first.astype(f32)
    second = rest.astype(bf16)
    third = (rest - second.astype(f32)).astype(bf16)
    digits = [(target // RADIX).astype(f32), (target % RADIX).astype(f32)]
    parts = digits + [first.astype(f32), second.astype(f32), third.astype(f32)]
    top = target.shape[1]
    spare = jnp.zeros((target.shape[0], SIDE - len(parts) * top), f32)
    out[:, :width] = tokens[...]
    out[:, width:] = jnp.concatenate(parts + [spare], 1).astype(bf16)


def packed(tokens, half, cap, *routing):
    count, top = routing[0].shape
    small = pl.BlockSpec((count, top), lambda i: (0, 0))
    return pl.pallas_call(
        lambda *refs: packed_body(cap, *refs),
        out_shape=jax.ShapeDtypeStruct((count, half + SIDE), bf16),
        grid=(1,),
        in_specs=[pl.BlockSpec((count, half), lambda i: (0, 0))] + [small] * len(routing),
        out_specs=pl.BlockSpec((count, half + SIDE), lambda i: (0, 0)),
        cost_estimate=cost(1e6, 6e5),
        name="packed",
    )(tokens, *routing)


def want_slots(shape, dim, base, block_of):
    slot = lax.broadcasted_iota(jnp.int32, shape, dim)
    place, source = slot & 7, (slot >> 3) & 1
    return (base + block_of(slot >> 4) * 8 + place).astype(f32) + SHIFT * source.astype(f32)


def keys_of(routes, top, dim):
    for k in range(top):
        take = (lambda n: routes[n : n + 1, :]) if dim == 1 else (lambda n: routes[:, n : n + 1])
        key = take(k) * RADIX + take(top + k)
        token = lax.broadcasted_iota(jnp.int32, key.shape, dim)
        half = routes.shape[dim] // PAIR
        yield k, key + SHIFT * (token // half).astype(f32)


def pick_body(top, scaled, base_ref, routes_ref, rows_ref, out_ref):
    slots = rows_ref.shape[0]
    routes = routes_ref[...].astype(f32).T
    want = want_slots((slots, slots), 0, base_ref[0], lambda block: block)
    chosen = jnp.zeros((slots, slots), f32)
    scale = jnp.zeros((slots, slots), f32)
    for k, key in keys_of(routes, top, 1):
        hit = key == want
        chosen = jnp.where(hit, 1.0, chosen)
        if scaled:
            part = lambda n: routes[n * top + k : n * top + k + 1, :]
            scale = jnp.where(hit, part(2) + part(3) + part(4), scale)
    picked = dot(chosen.astype(bf16), rows_ref[...])
    if scaled:
        picked = picked * jnp.sum(scale, axis=1, keepdims=True)
    out_ref[...] = picked.astype(bf16).reshape(out_ref.shape)


def pick(base, routed, rows, width, top, scaled, devices, experts, cap):
    slots = devices * experts * cap * PAIR
    steps = rows.shape[0] // slots
    return pl.pallas_call(
        lambda *refs: pick_body(top, scaled, *refs),
        out_shape=jax.ShapeDtypeStruct((devices, experts, steps * PAIR * cap, width), bf16),
        grid_spec=pltpu.PrefetchScalarGridSpec(
            num_scalar_prefetch=1,
            grid=(steps,),
            in_specs=[
                pl.BlockSpec((slots, SIDE), lambda i, b: (i, width // SIDE)),
                pl.BlockSpec((slots, width), lambda i, b: (i, 0)),
            ],
            out_specs=pl.BlockSpec(
                (devices, experts, PAIR * cap, width), lambda i, b: (0, 0, i, 0)
            ),
        ),
        cost_estimate=cost(2 * slots * slots * width * steps, 4 * slots * width * steps),
        name="pick_scaled" if scaled else "pick",
    )(base, routed, rows)


def give_back_body(top, base_ref, routes_ref, *refs):
    *row_refs, out_ref = refs
    slots = out_ref.shape[0]
    devices = len(row_refs)
    routes = routes_ref[...].astype(f32)
    here = base_ref[1]

    def block_of(block):
        return ((here - (block >> 1)) & (devices - 1)) * 2 + (block & 1)

    want = want_slots((slots, slots), 1, base_ref[0], block_of)
    chosen = jnp.zeros((slots, slots), f32)
    for _, key in keys_of(routes, top, 0):
        chosen = jnp.where(key == want, 1.0, chosen)
    width = out_ref.shape[1]
    rows = jnp.concatenate([r[...].reshape(slots // devices, width) for r in row_refs], 0)
    out_ref[...] = dot(chosen.astype(bf16), rows).astype(bf16)


def give_back(base, routed, pieces, top, cap):
    experts, all_rows, width = pieces[0].shape
    steps = all_rows // (PAIR * cap)
    slots = len(pieces) * experts * PAIR * cap
    return pl.pallas_call(
        lambda *refs: give_back_body(top, *refs),
        out_shape=jax.ShapeDtypeStruct((steps * slots, width), bf16),
        grid_spec=pltpu.PrefetchScalarGridSpec(
            num_scalar_prefetch=1,
            grid=(steps,),
            in_specs=[pl.BlockSpec((slots, SIDE), lambda i, b: (i, width // SIDE))]
            + [pl.BlockSpec((experts, PAIR * cap, width), lambda i, b: (0, i, 0))] * len(pieces),
            out_specs=pl.BlockSpec((slots, width), lambda i, b: (i, 0)),
        ),
        cost_estimate=cost(2 * slots * slots * width * steps, 4 * slots * width * steps),
        name="give_back",
    )(base, routed, *pieces)


def flat(ref):
    value = ref[...]
    return value.reshape(-1, value.shape[-1])


def forward_body(x0, x1, gate_w, up_w, proj, act, slope_up, hidden, x_proj):
    half = x0.shape[-1]
    rows = (flat(x0), flat(x1))

    def times(weight):
        return dot(rows[0], weight[:half]) + dot(rows[1], weight[half:])

    gate, upper = times(gate_w[0]), times(up_w[0])
    sigma = jax.nn.sigmoid(gate)
    activated = gate * sigma
    act[0] = activated
    slope_up[0] = upper * (sigma * (1.0 + gate * (1.0 - sigma)))
    hidden[0] = (activated * upper).astype(bf16)
    x_proj[0] = times(proj).astype(bf16)


def forward(x0, x1, gate_w, up_w, proj):
    plane, experts, depth, half = x0.shape
    width, hid = gate_w.shape[1:]
    rank = proj.shape[1]
    rows = plane * depth
    part = plane // 2
    row_spec = pl.BlockSpec((part, 1, depth, half), lambda j, s: (s, j, 0, 0))
    weight = pl.BlockSpec((1, width, hid), lambda j, s: (j, 0, 0))
    out = lambda n: pl.BlockSpec((1, part * depth, n), lambda j, s: (j, s, 0))
    shape = lambda n, t: jax.ShapeDtypeStruct((experts, rows, n), t)
    return pl.pallas_call(
        forward_body,
        out_shape=(shape(hid, f32), shape(hid, f32), shape(hid, bf16), shape(rank, bf16)),
        grid=(experts, 2),
        in_specs=[row_spec] * 2 + [weight] * 2 + [pl.BlockSpec((width, rank), lambda j, s: (0, 0))],
        out_specs=(out(hid), out(hid), out(hid), out(rank)),
        cost_estimate=cost(2 * experts * rows * width * (2 * hid + rank), 16e6),
        name="forward",
    )(x0, x1, gate_w, up_w, proj)


def first_half_body(dy, down_w, proj, hidden_grad, dy_proj):
    rows = flat(dy)
    hidden_grad[0] = dot(rows, down_w[0], ((1,), (1,)))
    dy_proj[0] = dot(rows, proj[...])


def first_half(dy, down_w, proj):
    plane, experts, depth, half = dy.shape
    hid, rank = down_w.shape[1], proj.shape[1]
    rows = plane * depth
    out = lambda n: pl.BlockSpec((1, rows, n), lambda j: (j, 0, 0))
    return pl.pallas_call(
        first_half_body,
        out_shape=tuple(jax.ShapeDtypeStruct((experts, rows, n), f32) for n in (hid, rank)),
        grid=(experts,),
        in_specs=[
            pl.BlockSpec((plane, 1, depth, half), lambda j: (0, j, 0, 0)),
            pl.BlockSpec((1, hid, half), lambda j: (j, 0, 0)),
            pl.BlockSpec((half, rank), lambda j: (0, 0)),
        ],
        out_specs=(out(hid), out(rank)),
        cost_estimate=cost(2 * experts * rows * half * (hid + rank), 8e6),
        name="first_half",
    )(dy, down_w, proj)


def backward_body(
    dy, down_w, proj, hidden_part, proj_part, act, slope_up, hidden, x_proj, gate_grad, up_grad, grads
):
    rows = flat(dy)
    hidden_grad = hidden_part[0] + dot(rows, down_w[0], ((1,), (1,)))
    dy_proj = (proj_part[0] + dot(rows, proj[...])).astype(bf16)
    of_up = (hidden_grad * act[0]).astype(bf16)
    of_gate = (hidden_grad * slope_up[0]).astype(bf16)
    up_grad[0] = of_up
    gate_grad[0] = of_gate
    over = ((0,), (0,))
    grads[0, 0] = dot(of_gate, x_proj[0], over).astype(bf16)
    grads[0, 1] = dot(of_up, x_proj[0], over).astype(bf16)
    grads[0, 2] = dot(hidden[0], dy_proj, over).astype(bf16)


def backward(dy, down_w, proj, hidden_part, proj_part, act, slope_up, hidden, x_proj):
    plane, experts, depth, half = dy.shape
    hid, rank = down_w.shape[1], proj.shape[1]
    rows = plane * depth
    mat = lambda n: pl.BlockSpec((1, rows, n), lambda j: (j, 0, 0))
    shape = jax.ShapeDtypeStruct((experts, rows, hid), bf16)
    return pl.pallas_call(
        backward_body,
        out_shape=(shape, shape, jax.ShapeDtypeStruct((experts, 3, hid, rank), bf16)),
        grid=(experts,),
        in_specs=[
            pl.BlockSpec((plane, 1, depth, half), lambda j: (0, j, 0, 0)),
            pl.BlockSpec((1, hid, half), lambda j: (j, 0, 1)),
            pl.BlockSpec((half, rank), lambda j: (1, 0)),
            mat(hid), mat(rank), mat(hid), mat(hid), mat(hid), mat(rank),
        ],
        out_specs=(mat(hid), mat(hid), pl.BlockSpec((1, 3, hid, rank), lambda j: (j, 0, 0, 0))),
        cost_estimate=cost(2 * experts * rows * (half * (hid + rank) + 3 * hid * rank), 12e6),
        name="backward",
    )(dy, down_w, proj, hidden_part, proj_part, act, slope_up, hidden, x_proj)


def row_grads_body(gate_grad, up_grad, gate_w, up_w, out0, out1):
    half = out0.shape[-1]
    over = ((1,), (1,))
    for n, out in enumerate((out0, out1)):
        part = slice(n * half, (n + 1) * half)
        value = dot(gate_grad[0], gate_w[0, part], over) + dot(up_grad[0], up_w[0, part], over)
        out[...] = value.astype(bf16).reshape(out.shape)


def row_grads_of(gate_grad, up_grad, gate_w, up_w, plane):
    experts, rows, hid = gate_grad.shape
    width = gate_w.shape[1]
    depth, part = rows // plane, plane // 2
    mat = pl.BlockSpec((1, rows // 2, hid), lambda j, s: (j, s, 0))
    weight = pl.BlockSpec((1, width, hid), lambda j, s: (j, 0, 0))
    shape = jax.ShapeDtypeStruct((plane, experts, depth, width // 2), bf16)
    return pl.pallas_call(
        row_grads_body,
        out_shape=(shape, shape),
        grid=(experts, 2),
        in_specs=[mat, mat, weight, weight],
        out_specs=[pl.BlockSpec((part, 1, depth, width // 2), lambda j, s: (s, j, 0, 0))] * 2,
        cost_estimate=cost(4 * experts * rows * width * hid, 12e6),
        name="row_grads",
    )(gate_grad, up_grad, gate_w, up_w)


def weight_grads_body(x0, x1, dy0, dy1, gate_grad, up_grad, hidden, out):
    half, hid = x0.shape[-1], hidden.shape[-1]
    over = ((0,), (0,))
    for n, (x, dy) in enumerate(((x0, dy0), (x1, dy1))):
        part = pl.ds(n * half, half)
        out[part, 0:hid] = dot(flat(x), gate_grad[0], over).astype(bf16)
        out[part, hid : 2 * hid] = dot(flat(x), up_grad[0], over).astype(bf16)
        out[part, 2 * hid : 3 * hid] = dot(flat(dy), hidden[0], over).astype(bf16)


def weight_grads(x0, x1, dy0, dy1, gate_grad, up_grad, hidden):
    plane, experts, depth, half = x0.shape
    rows, hid = plane * depth, hidden.shape[2]
    row_spec = pl.BlockSpec((plane, 1, depth, half), lambda j: (0, j, 0, 0))
    mat = pl.BlockSpec((1, rows, hid), lambda j: (j, 0, 0))
    return pl.pallas_call(
        weight_grads_body,
        out_shape=jax.ShapeDtypeStruct((2 * half, 3 * hid * experts), bf16),
        grid=(experts,),
        in_specs=[row_spec] * 4 + [mat] * 3,
        out_specs=pl.BlockSpec((2 * half, 3 * hid), lambda j: (0, j)),
        cost_estimate=cost(12 * experts * rows * half * hid, 24e6),
        name="weight_grads",
    )(x0, x1, dy0, dy1, gate_grad, up_grad, hidden)


def inverse_factor(square):
    size = square.shape[0]
    row = lax.broadcasted_iota(jnp.int32, (size, 2 * size), 0)
    lane = lax.broadcasted_iota(jnp.int32, (size, 2 * size), 1)
    work = jnp.concatenate([square, jnp.zeros_like(square)], 1)
    work = jnp.where(lane == row + size, 1.0, work)
    groups = [work[g : g + 8] for g in range(0, size, 8)]
    scales = [jnp.zeros((8, 2 * size), f32) for _ in groups]
    inner = lax.broadcasted_iota(jnp.int32, (8, 2 * size), 0)
    for j in range(size):
        g, at = divmod(j, 8)
        spread = [jnp.broadcast_to(w[:, j : j + 1], (8, 2 * size)) for w in groups[g:]]
        pivot = spread[0][at : at + 1]
        line = groups[g][at : at + 1]
        scales[g] = jnp.where(inner == at, lax.rsqrt(pivot), scales[g])
        line = line / pivot
        factor = jnp.where(inner > at, spread[0], 0.0)
        groups[g] = groups[g] - factor * line
        for n in range(g + 1, len(groups)):
            groups[n] = groups[n] - spread[n - g] * line
    return jnp.concatenate([w * s for w, s in zip(groups, scales)], 0)


def new_basis_body(scale, index_ref, power, own, out, gram, side, solved):
    size = power.shape[1]
    exact = lax.Precision.HIGHEST
    over = ((0,), (0,))
    gram[...] = dot(power[...], power[...], over)
    panel = own[...].astype(f32)
    spare = jnp.zeros((SIDE - panel.shape[0], size), f32)
    side[...] = jnp.concatenate([panel, spare], 0).T

    def step(k, _):
        head = gram[0:BLOCK]
        factor = inverse_factor(head[:, 0:BLOCK])
        none = jnp.zeros_like(head)
        lines = dot(factor, jnp.concatenate([none, head], 0), precision=exact)
        head = side[0:BLOCK]
        answer = dot(factor, jnp.concatenate([jnp.zeros_like(head), head], 0), precision=exact)
        solved[pl.ds(pl.multiple_of(k * BLOCK, BLOCK), BLOCK)] = answer
        lower = lines[:, BLOCK:]
        rest = gram[BLOCK:] - dot(lower, lines, over, exact)
        rest = jnp.concatenate([rest[:, BLOCK:], jnp.zeros((size - BLOCK, BLOCK), f32)], 1)
        gram[0 : size - BLOCK] = rest
        side[0 : size - BLOCK] = side[BLOCK:] - dot(lower, answer, over, exact)
        return 0

    lax.fori_loop(0, size // BLOCK, step, 0)
    out[...] = scale * solved[...].T[: out.shape[0]]


def new_basis_of(power, index, panel_rows):
    width, rank = power.shape
    return pl.pallas_call(
        lambda *refs: new_basis_body(math.sqrt(width), *refs),
        out_shape=jax.ShapeDtypeStruct((panel_rows, rank), f32),
        grid_spec=pltpu.PrefetchScalarGridSpec(
            num_scalar_prefetch=1,
            grid=(1,),
            in_specs=[
                pl.BlockSpec((width, rank), lambda i, n: (0, 0)),
                pl.BlockSpec((panel_rows, rank), lambda i, n: (n[0], 0)),
            ],
            out_specs=pl.BlockSpec((panel_rows, rank), lambda i, n: (0, 0)),
            scratch_shapes=[
                pltpu.VMEM((rank, rank), f32),
                pltpu.VMEM((rank, SIDE), f32),
                pltpu.VMEM((rank, SIDE), f32),
            ],
        ),
        cost_estimate=cost(3e10, 2e6),
        name="new_basis",
    )(index, power, power)


def layer(
    tokens,
    cotangent,
    route_weights,
    expert_ids,
    slot_ids,
    kept_mask,
    gate_weight,
    up_weight,
    down_weight,
    projector_basis,
):
    tok_count, model_width = tokens.shape
    half = model_width // 2
    top = expert_ids.shape[1]
    experts = gate_weight.shape[0]
    group_count = lax.axis_size(EXPERT)
    plane = lax.axis_size(PLANE)
    cap = tok_count * top // (experts * group_count)
    here = lax.axis_index(PLANE)
    base = jnp.stack([lax.axis_index(Z) * (plane * experts * cap), here]).astype(jnp.int32)

    first_rows = packed(tokens, half, cap, expert_ids, slot_ids, kept_mask, route_weights)

    def along_z(value):
        return lax.all_gather(value, Z, axis=0, tiled=True)

    def after(value, *earlier):
        return lax.optimization_barrier((value, *earlier))

    projector = (projector_basis * (1.0 / math.sqrt(model_width))).astype(bf16)
    projector = gathered(projector, (Z, X))
    pieces = from_everyone(projector, C)
    pieces = pieces.reshape(lax.axis_size(C), -1, *projector_basis.shape).swapaxes(0, 1)
    projector = pieces.reshape(model_width, -1)

    x0_all = along_z(first_rows)
    x1_in, x0_all, projector = after(tokens[:, half:], x0_all, projector)
    x1_all = along_z(x1_in)
    dy0_in, x1_all = after(cotangent[:, :half], x1_all)
    dy0_all = along_z(dy0_in)
    dy1_in, dy0_all = after(cotangent[:, half:], dy0_all)
    dy1_all = along_z(dy1_in)

    def sent(rows, scaled):
        picked = pick(base, x0_all, rows, half, top, scaled, plane, experts, cap)
        return lax.all_to_all(picked, PLANE, split_axis=0, concat_axis=0, tiled=True)

    x0, x1 = sent(x0_all, False), sent(x1_all, False)
    dy0, dy1 = sent(dy0_all, True), sent(dy1_all, True)

    act, slope_up, hidden, x_proj = forward(x0, x1, gate_weight, up_weight, projector)
    hidden_part, proj_part = first_half(dy0, down_weight, projector)
    gate_grad, up_grad, partial = backward(
        dy1, down_weight, projector, hidden_part, proj_part, act, slope_up, hidden, x_proj
    )

    own_grads = sent_and_summed(partial.reshape(-1, partial.shape[-1]), Y)
    grads_low = gathered(own_grads, Y)
    projected_grads = grads_low.astype(f32).reshape(partial.shape)

    returned = []
    halves = row_grads_of(gate_grad, up_grad, gate_weight, up_weight, plane)
    for rows in halves:
        pieces = []
        for d in range(plane):
            piece = lax.dynamic_index_in_dim(rows, (here + d) % plane, 0, keepdims=False)
            if d:
                piece = lax.ppermute(piece, PLANE, [(i, (i + d) % plane) for i in range(plane)])
            pieces.append(piece)
        returned.append(pieces)

    late_gate_grad, _ = after(gate_grad, own_grads)
    own_weight_grads = weight_grads(x0, x1, dy0, dy1, late_gate_grad, up_grad, hidden)
    near, far = (C, Y), (Z, X)
    power = dot(own_weight_grads, grads_low).astype(bf16)
    first_base, power = after(base, power)
    power = sent_and_summed(power, near)
    second_base, power = after(base, power)
    power = sent_and_summed(power, far)
    power = gathered(gathered(power, far), near)

    token_parts = []
    for when, pieces in zip((first_base, second_base), returned):
        token_parts.append(give_back(when, x0_all, pieces, top, cap))
    token_grads = jnp.concatenate(
        [lax.psum_scatter(part, Z, scatter_dimension=0, tiled=True) for part in token_parts], 1
    )

    index = lax.axis_index(EXPERT).astype(jnp.int32).reshape(1)
    new_basis = new_basis_of(power, index, model_width // group_count)
    return (token_grads, projected_grads, new_basis)


def solution(mesh):
    finer = Mesh(mesh.devices.reshape(8, 4, 2, mesh.shape["replica"]), EXPERT_REPLICA)
    rows = P(EXPERT_REPLICA, None)
    placed = (rows,) * 6 + (P(EXPERT, None, None),) * 3 + (P(EXPERT, None),)
    return jax.shard_map(
        layer,
        mesh=finer,
        in_specs=placed,
        out_specs=(rows, P(EXPERT, None, None, None), P(EXPERT, None)),
        check_vma=False,
    )
```

```python
import math

import jax
import jax.numpy as jnp
from jax import lax
from jax.experimental import pallas as pl
from jax.experimental.pallas import tpu as pltpu
from jax.sharding import Mesh
from jax.sharding import PartitionSpec as P

Z, X, C, Y = "expert_0", "expert_1", "expert_2", "replica"
EXPERT = (Z, X, C)
EXPERT_REPLICA = (Z, X, C, Y)
PLANE = (X, C)
PAIR = 2
RADIX = 256
DROPPED = 255 * RADIX
SHIFT = float(1 << 17)
SIDE = 128
BLOCK = 64


f32, bf16 = jnp.float32, jnp.bfloat16


def dot(a, b, over=((1,), (0,)), precision=None):
    return lax.dot_general(a, b, (over, ((), ())), precision=precision, preferred_element_type=f32)


def cost(flops, nbytes):
    return pl.CostEstimate(flops=int(flops), bytes_accessed=int(nbytes), transcendentals=0)


def from_everyone(array, axis):
    copies = jnp.broadcast_to(array, (lax.axis_size(axis), *array.shape))
    return lax.all_to_all(copies, axis, split_axis=0, concat_axis=0, tiled=True)


def sent_and_summed(lines, axis):
    devices = lax.axis_size(axis)
    pieces = lines.reshape(devices, -1, lines.shape[-1])
    arrived = lax.all_to_all(pieces, axis, split_axis=0, concat_axis=0, tiled=True)
    return arrived.astype(f32).sum(axis=0).astype(bf16)


def sum_and_spread_body(arrived, out):
    total = arrived[...].astype(f32).sum(axis=0).astype(bf16)
    out[...] = jnp.broadcast_to(total[None], out.shape)


def sum_and_spread(arrived, steps):
    devices, lines, width = arrived.shape
    spec = pl.BlockSpec((devices, lines // steps, width), lambda i: (0, i, 0))
    return pl.pallas_call(
        sum_and_spread_body,
        out_shape=jax.ShapeDtypeStruct(arrived.shape, bf16),
        grid=(steps,),
        in_specs=[spec],
        out_specs=spec,
        cost_estimate=cost(arrived.size, 4 * arrived.size),
        compiler_params=pltpu.CompilerParams(vmem_limit_bytes=8 * 2**20),
        name="sum_and_spread",
    )(arrived)


def exchanged(pieces, axis):
    return lax.all_to_all(pieces, axis, split_axis=0, concat_axis=0, tiled=True)


def gathered(lines, axis):
    return from_everyone(lines, axis).reshape(-1, lines.shape[-1])


def packed_body(cap, tokens, expert_ids, slot_ids, kept_mask, route_weights, out):
    width = tokens.shape[1]
    target = jnp.where(kept_mask[...] > 0, expert_ids[...] * cap + slot_ids[...], DROPPED)
    weight = route_weights[...]
    first = weight.astype(bf16)
    rest = weight - first.astype(f32)
    second = rest.astype(bf16)
    third = (rest - second.astype(f32)).astype(bf16)
    digits = [(target // RADIX).astype(f32), (target % RADIX).astype(f32)]
    parts = digits + [first.astype(f32), second.astype(f32), third.astype(f32)]
    top = target.shape[0]
    spare = jnp.zeros((SIDE - len(parts) * top, target.shape[1]), f32)
    out[:, :width] = tokens[...]
    out[:, width:] = jnp.concatenate(parts + [spare], 0).T.astype(bf16)


def packed(tokens, cap, *routing):
    count, width = tokens.shape
    return pl.pallas_call(
        lambda *refs: packed_body(cap, *refs),
        out_shape=jax.ShapeDtypeStruct((count, width + SIDE), bf16),
        cost_estimate=cost(1e6, 6e5),
        name="packed",
    )(tokens, *(array.T for array in routing))


def want_slots(shape, dim, base, block_of):
    slot = lax.broadcasted_iota(jnp.int32, shape, dim)
    place, source = slot & 7, (slot >> 3) & 1
    return (base + block_of(slot >> 4) * 8 + place).astype(f32) + SHIFT * source.astype(f32)


def keys_of(routes, top, dim):
    for k in range(top):
        take = (lambda n: routes[n : n + 1, :]) if dim == 1 else (lambda n: routes[:, n : n + 1])
        key = take(k) * RADIX + take(top + k)
        token = lax.broadcasted_iota(jnp.int32, key.shape, dim)
        half = routes.shape[dim] // PAIR
        yield k, key + SHIFT * (token // half).astype(f32)


def pick_body(top, scaled, base_ref, routes_ref, rows_ref, out_ref):
    slots = rows_ref.shape[0]
    routes = routes_ref[...].astype(f32).T
    want = want_slots((slots, slots), 0, base_ref[0], lambda block: block)
    chosen = jnp.zeros((slots, slots), f32)
    scale = jnp.zeros((slots, slots), f32)
    for k, key in keys_of(routes, top, 1):
        hit = key == want
        chosen = jnp.where(hit, 1.0, chosen)
        if scaled:
            part = lambda n: routes[n * top + k : n * top + k + 1, :]
            scale = jnp.where(hit, part(2) + part(3) + part(4), scale)
    picked = dot(chosen.astype(bf16), rows_ref[...])
    if scaled:
        picked = picked * jnp.sum(scale, axis=1, keepdims=True)
    out_ref[...] = picked.astype(bf16).reshape(out_ref.shape)


def pick(base, routed, rows, width, top, scaled, devices, experts, cap):
    slots = devices * experts * cap * PAIR
    steps = rows.shape[0] // slots
    return pl.pallas_call(
        lambda *refs: pick_body(top, scaled, *refs),
        out_shape=jax.ShapeDtypeStruct((devices, experts, steps * PAIR * cap, width), bf16),
        grid_spec=pltpu.PrefetchScalarGridSpec(
            num_scalar_prefetch=1,
            grid=(steps,),
            in_specs=[
                pl.BlockSpec((slots, SIDE), lambda i, b: (i, width // SIDE)),
                pl.BlockSpec((slots, width), lambda i, b: (i, 0)),
            ],
            out_specs=pl.BlockSpec(
                (devices, experts, PAIR * cap, width), lambda i, b: (0, 0, i, 0)
            ),
        ),
        cost_estimate=cost(2 * slots * slots * width * steps, 4 * slots * width * steps),
        name="pick_scaled" if scaled else "pick",
    )(base, routed, rows)


def give_back_body(top, base_ref, routes_ref, *refs):
    *row_refs, out_ref = refs
    slots = out_ref.shape[0]
    devices = len(row_refs)
    routes = routes_ref[...].astype(f32)
    here = base_ref[1]

    def block_of(block):
        return ((here - (block >> 1)) & (devices - 1)) * 2 + (block & 1)

    want = want_slots((slots, slots), 1, base_ref[0], block_of)
    chosen = jnp.zeros((slots, slots), f32)
    for _, key in keys_of(routes, top, 0):
        chosen = jnp.where(key == want, 1.0, chosen)
    width = out_ref.shape[1]
    rows = jnp.concatenate([r[...].reshape(slots // devices, width) for r in row_refs], 0)
    out_ref[...] = dot(chosen.astype(bf16), rows).astype(bf16)


def give_back(base, routed, pieces, top, cap):
    experts, all_rows, width = pieces[0].shape
    steps = all_rows // (PAIR * cap)
    slots = len(pieces) * experts * PAIR * cap
    return pl.pallas_call(
        lambda *refs: give_back_body(top, *refs),
        out_shape=jax.ShapeDtypeStruct((steps * slots, width), bf16),
        grid_spec=pltpu.PrefetchScalarGridSpec(
            num_scalar_prefetch=1,
            grid=(steps,),
            in_specs=[pl.BlockSpec((slots, SIDE), lambda i, b: (i, width // SIDE))]
            + [pl.BlockSpec((experts, PAIR * cap, width), lambda i, b: (0, i, 0))] * len(pieces),
            out_specs=pl.BlockSpec((slots, width), lambda i, b: (i, 0)),
        ),
        cost_estimate=cost(2 * slots * slots * width * steps, 4 * slots * width * steps),
        name="give_back",
    )(base, routed, *pieces)


def flat(ref):
    value = ref[...]
    return value.reshape(-1, value.shape[-1])


def forward_body(x, gate_w, up_w, proj, act, slope_up, hidden, x_proj):
    rows = flat(x)
    gate, upper = dot(rows, gate_w[0]), dot(rows, up_w[0])
    sigma = jax.nn.sigmoid(gate)
    activated = gate * sigma
    act[0] = activated
    slope_up[0] = upper * (sigma * (1.0 + gate * (1.0 - sigma)))
    hidden[0] = (activated * upper).astype(bf16)
    x_proj[0] = dot(rows, proj[...]).astype(bf16)


def forward(x, gate_w, up_w, proj):
    plane, experts, depth, width = x.shape
    hid, rank = gate_w.shape[2], proj.shape[1]
    rows = plane * depth
    part = plane // 2
    weight = pl.BlockSpec((1, width, hid), lambda j, s: (j, 0, 0))
    out = lambda n: pl.BlockSpec((1, part * depth, n), lambda j, s: (j, s, 0))
    shape = lambda n, t: jax.ShapeDtypeStruct((experts, rows, n), t)
    return pl.pallas_call(
        forward_body,
        out_shape=(shape(hid, f32), shape(hid, f32), shape(hid, bf16), shape(rank, bf16)),
        grid=(experts, 2),
        in_specs=[pl.BlockSpec((part, 1, depth, width), lambda j, s: (s, j, 0, 0))]
        + [weight] * 2
        + [pl.BlockSpec((width, rank), lambda j, s: (0, 0))],
        out_specs=(out(hid), out(hid), out(hid), out(rank)),
        cost_estimate=cost(2 * experts * rows * width * (2 * hid + rank), 16e6),
        name="forward",
    )(x, gate_w, up_w, proj)


def backward_body(dy, down_w, proj, act, slope_up, hidden, x_proj, gate_grad, up_grad, grads):
    rows = flat(dy)
    hidden_grad = dot(rows, down_w[0], ((1,), (1,)))
    dy_proj = dot(rows, proj[...]).astype(bf16)
    of_up = (hidden_grad * act[0]).astype(bf16)
    of_gate = (hidden_grad * slope_up[0]).astype(bf16)
    up_grad[0] = of_up
    gate_grad[0] = of_gate
    over = ((0,), (0,))
    grads[0, 0] = dot(of_gate, x_proj[0], over).astype(bf16)
    grads[0, 1] = dot(of_up, x_proj[0], over).astype(bf16)
    grads[0, 2] = dot(hidden[0], dy_proj, over).astype(bf16)


def backward(dy, down_w, proj, act, slope_up, hidden, x_proj):
    plane, experts, depth, width = dy.shape
    hid, rank = down_w.shape[1], proj.shape[1]
    rows = plane * depth
    mat = lambda n: pl.BlockSpec((1, rows, n), lambda j: (j, 0, 0))
    shape = jax.ShapeDtypeStruct((experts, rows, hid), bf16)
    return pl.pallas_call(
        backward_body,
        out_shape=(shape, shape, jax.ShapeDtypeStruct((experts, 3, hid, rank), bf16)),
        grid=(experts,),
        in_specs=[
            pl.BlockSpec((plane, 1, depth, width), lambda j: (0, j, 0, 0)),
            pl.BlockSpec((1, hid, width), lambda j: (j, 0, 0)),
            pl.BlockSpec((width, rank), lambda j: (0, 0)),
            mat(hid), mat(hid), mat(hid), mat(rank),
        ],
        out_specs=(mat(hid), mat(hid), pl.BlockSpec((1, 3, hid, rank), lambda j: (j, 0, 0, 0))),
        cost_estimate=cost(2 * experts * rows * (width * (hid + rank) + 3 * hid * rank), 16e6),
        name="backward",
    )(dy, down_w, proj, act, slope_up, hidden, x_proj)


def row_grads_body(gate_grad, up_grad, gate_w, up_w, out):
    over = ((1,), (1,))
    value = dot(gate_grad[0], gate_w[0], over) + dot(up_grad[0], up_w[0], over)
    out[...] = value.astype(bf16).reshape(out.shape)


def row_grads_of(gate_grad, up_grad, gate_w, up_w, plane):
    experts, rows, hid = gate_grad.shape
    width = gate_w.shape[1]
    depth, part = rows // plane, plane // 2
    mat = pl.BlockSpec((1, rows // 2, hid), lambda j, s: (j, s, 0))
    weight = pl.BlockSpec((1, width, hid), lambda j, s: (j, 0, 0))
    return pl.pallas_call(
        row_grads_body,
        out_shape=jax.ShapeDtypeStruct((plane, experts, depth, width), bf16),
        grid=(experts, 2),
        in_specs=[mat, mat, weight, weight],
        out_specs=pl.BlockSpec((part, 1, depth, width), lambda j, s: (s, j, 0, 0)),
        cost_estimate=cost(4 * experts * rows * width * hid, 12e6),
        name="row_grads",
    )(gate_grad, up_grad, gate_w, up_w)


def weight_grads_body(x, dy, gate_grad, up_grad, hidden, out):
    hid = hidden.shape[-1]
    over = ((0,), (0,))
    out[:, 0:hid] = dot(flat(x), gate_grad[0], over).astype(bf16)
    out[:, hid : 2 * hid] = dot(flat(x), up_grad[0], over).astype(bf16)
    out[:, 2 * hid : 3 * hid] = dot(flat(dy), hidden[0], over).astype(bf16)


def weight_grads(x, dy, gate_grad, up_grad, hidden):
    plane, experts, depth, width = x.shape
    rows, hid = plane * depth, hidden.shape[2]
    part = width // 2
    row_spec = pl.BlockSpec((plane, 1, depth, part), lambda j, n: (0, j, 0, n))
    mat = pl.BlockSpec((1, rows, hid), lambda j, n: (j, 0, 0))
    return pl.pallas_call(
        weight_grads_body,
        out_shape=jax.ShapeDtypeStruct((width, 3 * hid * experts), bf16),
        grid=(experts, 2),
        in_specs=[row_spec] * 2 + [mat] * 3,
        out_specs=pl.BlockSpec((part, 3 * hid), lambda j, n: (n, j)),
        cost_estimate=cost(6 * experts * rows * width * hid, 24e6),
        compiler_params=pltpu.CompilerParams(vmem_limit_bytes=36 * 2**20),
        name="weight_grads",
    )(x, dy, gate_grad, up_grad, hidden)


def power_body(weights, grads, out):
    out[...] = dot(weights[...], grads[...]).astype(bf16)


def power_of(weights, grads):
    width, depth = weights.shape
    rank = grads.shape[1]
    part = width // 8
    return pl.pallas_call(
        power_body,
        out_shape=jax.ShapeDtypeStruct((width, rank), bf16),
        grid=(8,),
        in_specs=[
            pl.BlockSpec((part, depth), lambda i: (i, 0)),
            pl.BlockSpec((depth, rank), lambda i: (0, 0)),
        ],
        out_specs=pl.BlockSpec((part, rank), lambda i: (i, 0)),
        cost_estimate=cost(2 * width * depth * rank, 12e6),
        compiler_params=pltpu.CompilerParams(vmem_limit_bytes=20 * 2**20),
        name="power",
    )(weights, grads)


def inverse_factor(square):
    size = square.shape[0]
    row = lax.broadcasted_iota(jnp.int32, (size, 2 * size), 0)
    lane = lax.broadcasted_iota(jnp.int32, (size, 2 * size), 1)
    work = jnp.concatenate([square, jnp.zeros_like(square)], 1)
    work = jnp.where(lane == row + size, 1.0, work)
    groups = [work[g : g + 8] for g in range(0, size, 8)]
    scales = [jnp.zeros((8, 2 * size), f32) for _ in groups]
    inner = lax.broadcasted_iota(jnp.int32, (8, 2 * size), 0)
    for j in range(0, size, 2):
        g, at = divmod(j, 8)
        spread = [jnp.broadcast_to(w[:, j : j + 1], (8, 2 * size)) for w in groups[g:]]
        beside = [jnp.broadcast_to(w[:, j + 1 : j + 2], (8, 2 * size)) for w in groups[g:]]
        pivot, under = spread[0][at : at + 1], spread[0][at + 1 : at + 2]
        share = 1.0 / pivot
        line = groups[g][at : at + 1] * share
        across = beside[0][at : at + 1] * share
        next_pivot = beside[0][at + 1 : at + 2] - under * across
        next_line = (groups[g][at + 1 : at + 2] - under * line) / next_pivot
        scale = jnp.where(inner == at + 1, lax.rsqrt(next_pivot), scales[g])
        scales[g] = jnp.where(inner == at, lax.rsqrt(pivot), scale)
        for n in range(g, len(groups)):
            first, second = spread[n - g], beside[n - g] - spread[n - g] * across
            if n == g:
                first = jnp.where(inner > at, first, 0.0)
                second = jnp.where(inner > at + 1, second, 0.0)
            groups[n] = groups[n] - first * line - second * next_line
    return jnp.concatenate([w * s for w, s in zip(groups, scales)], 0)


def new_basis_body(scale, index_ref, power, own, out, gram, side, solved):
    size = power.shape[1]
    exact = lax.Precision.HIGHEST
    over = ((0,), (0,))
    gram[...] = dot(power[...], power[...], over)
    panel = own[...].astype(f32)
    spare = jnp.zeros((SIDE - panel.shape[0], size), f32)
    side[...] = jnp.concatenate([panel, spare], 0).T

    def step(k, _):
        head = gram[0:BLOCK]
        factor = inverse_factor(head[:, 0:BLOCK])
        none = jnp.zeros_like(head)
        lines = dot(factor, jnp.concatenate([none, head], 0), precision=exact)
        head = side[0:BLOCK]
        answer = dot(factor, jnp.concatenate([jnp.zeros_like(head), head], 0), precision=exact)
        solved[pl.ds(pl.multiple_of(k * BLOCK, BLOCK), BLOCK)] = answer
        lower = lines[:, BLOCK:]
        rest = gram[BLOCK:] - dot(lower, lines, over, exact)
        rest = jnp.concatenate([rest[:, BLOCK:], jnp.zeros((size - BLOCK, BLOCK), f32)], 1)
        gram[0 : size - BLOCK] = rest
        side[0 : size - BLOCK] = side[BLOCK:] - dot(lower, answer, over, exact)
        return 0

    lax.fori_loop(0, size // BLOCK, step, 0)
    out[...] = scale * solved[...].T[: out.shape[0]]


def new_basis_of(power, index, panel_rows):
    width, rank = power.shape
    return pl.pallas_call(
        lambda *refs: new_basis_body(math.sqrt(width), *refs),
        out_shape=jax.ShapeDtypeStruct((panel_rows, rank), f32),
        grid_spec=pltpu.PrefetchScalarGridSpec(
            num_scalar_prefetch=1,
            grid=(1,),
            in_specs=[
                pl.BlockSpec((width, rank), lambda i, n: (0, 0)),
                pl.BlockSpec((panel_rows, rank), lambda i, n: (n[0], 0)),
            ],
            out_specs=pl.BlockSpec((panel_rows, rank), lambda i, n: (0, 0)),
            scratch_shapes=[
                pltpu.VMEM((rank, rank), f32),
                pltpu.VMEM((rank, SIDE), f32),
                pltpu.VMEM((rank, SIDE), f32),
            ],
        ),
        cost_estimate=cost(3e10, 2e6),
        compiler_params=pltpu.CompilerParams(vmem_limit_bytes=24 * 2**20),
        name="new_basis",
    )(index, power, power)


def layer(
    tokens,
    cotangent,
    route_weights,
    expert_ids,
    slot_ids,
    kept_mask,
    gate_weight,
    up_weight,
    down_weight,
    projector_basis,
):
    tok_count, model_width = tokens.shape
    top = expert_ids.shape[1]
    experts = gate_weight.shape[0]
    group_count = lax.axis_size(EXPERT)
    plane = lax.axis_size(PLANE)
    cap = tok_count * top // (experts * group_count)
    here = lax.axis_index(PLANE)
    base = jnp.stack([lax.axis_index(Z) * (plane * experts * cap), here]).astype(jnp.int32)

    def along_z(value):
        return lax.all_gather(value, Z, axis=0, tiled=True)

    def after(value, *earlier):
        return lax.optimization_barrier((value, *earlier))

    projector = (projector_basis * (1.0 / math.sqrt(model_width))).astype(bf16)
    projector = gathered(projector, (Z, X))
    first_rows = packed(tokens, cap, expert_ids, slot_ids, kept_mask, route_weights)
    first_rows, projector = after(first_rows, projector)
    pieces = from_everyone(projector, C)
    pieces = pieces.reshape(lax.axis_size(C), -1, *projector_basis.shape).swapaxes(0, 1)
    projector = pieces.reshape(model_width, -1)

    x_all = along_z(first_rows)
    dy_in, x_all, projector = after(cotangent, x_all, projector)
    dy_all = along_z(dy_in)

    def sent(rows, scaled):
        picked = pick(base, x_all, rows, model_width, top, scaled, plane, experts, cap)
        return lax.all_to_all(picked, PLANE, split_axis=0, concat_axis=0, tiled=True)

    x, dy = sent(x_all, False), sent(dy_all, True)
    act, slope_up, hidden, x_proj = forward(x, gate_weight, up_weight, projector)
    gate_grad, up_grad, partial = backward(
        dy, down_weight, projector, act, slope_up, hidden, x_proj
    )

    replicas = lax.axis_size(Y)
    arrived = exchanged(partial.reshape(replicas, -1, partial.shape[-1]), Y)
    spread = sum_and_spread(arrived, 3)
    grads_low = exchanged(spread, Y)
    projected_grads = grads_low.astype(f32).reshape(partial.shape)
    grads_low = grads_low.reshape(-1, partial.shape[-1])

    rows = row_grads_of(gate_grad, up_grad, gate_weight, up_weight, plane)
    returned = []
    for d in range(plane):
        piece = lax.dynamic_index_in_dim(rows, (here + d) % plane, 0, keepdims=False)
        if d:
            piece = lax.ppermute(piece, PLANE, [(i, (i + d) % plane) for i in range(plane)])
        returned.append(piece)

    late_gate_grad, _ = after(gate_grad, spread)
    own_weight_grads = weight_grads(x, dy, late_gate_grad, up_grad, hidden)
    near, far = (C, Y), (Z, X)
    power = power_of(own_weight_grads, grads_low)
    late_base, power = after(base, power)
    power = sent_and_summed(power, near)
    power = exchanged(power.reshape(lax.axis_size(far), -1, power.shape[-1]), far)
    power = exchanged(sum_and_spread(power, 1), far).reshape(-1, power.shape[-1])
    power = gathered(power, near)

    token_parts = give_back(late_base, x_all, returned, top, cap)
    token_grads = lax.psum_scatter(token_parts, Z, scatter_dimension=0, tiled=True)

    index = lax.axis_index(EXPERT).astype(jnp.int32).reshape(1)
    new_basis = new_basis_of(power, index, model_width // group_count)
    return (token_grads, projected_grads, new_basis)


def solution(mesh):
    finer = Mesh(mesh.devices.reshape(8, 4, 2, mesh.shape["replica"]), EXPERT_REPLICA)
    rows = P(EXPERT_REPLICA, None)
    placed = (rows,) * 6 + (P(EXPERT, None, None),) * 3 + (P(EXPERT, None),)
    return jax.shard_map(
        layer,
        mesh=finer,
        in_specs=placed,
        out_specs=(rows, P(EXPERT, None, None, None), P(EXPERT, None)),
        check_vma=False,
    )
```

```python
import math

import jax
import jax.numpy as jnp
from jax import lax
from jax.experimental import pallas as pl
from jax.experimental.pallas import tpu as pltpu
from jax.sharding import Mesh
from jax.sharding import PartitionSpec as P

Z, X, C, Y = "expert_0", "expert_1", "expert_2", "replica"
EXPERT = (Z, X, C)
EXPERT_REPLICA = (Z, X, C, Y)
PLANE = (X, C)
PAIR = 2
RADIX = 256
DROPPED = 255 * RADIX
SHIFT = float(1 << 17)
SIDE = 128
BLOCK = 64


f32, bf16 = jnp.float32, jnp.bfloat16


def dot(a, b, over=((1,), (0,)), precision=None):
    return lax.dot_general(a, b, (over, ((), ())), precision=precision, preferred_element_type=f32)


def cost(flops, nbytes):
    return pl.CostEstimate(flops=int(flops), bytes_accessed=int(nbytes), transcendentals=0)


def from_everyone(array, axis):
    copies = jnp.broadcast_to(array, (lax.axis_size(axis), *array.shape))
    return lax.all_to_all(copies, axis, split_axis=0, concat_axis=0, tiled=True)


def sent_and_summed(lines, axis):
    devices = lax.axis_size(axis)
    pieces = lines.reshape(devices, -1, lines.shape[-1])
    arrived = lax.all_to_all(pieces, axis, split_axis=0, concat_axis=0, tiled=True)
    return arrived.astype(f32).sum(axis=0).astype(bf16)


def sum_and_spread_body(arrived, out):
    total = arrived[...].astype(f32).sum(axis=0).astype(bf16)
    out[...] = jnp.broadcast_to(total[None], out.shape)


def sum_and_spread(arrived, steps):
    devices, lines, width = arrived.shape
    spec = pl.BlockSpec((devices, lines // steps, width), lambda i: (0, i, 0))
    return pl.pallas_call(
        sum_and_spread_body,
        out_shape=jax.ShapeDtypeStruct(arrived.shape, bf16),
        grid=(steps,),
        in_specs=[spec],
        out_specs=spec,
        cost_estimate=cost(arrived.size, 4 * arrived.size),
        compiler_params=pltpu.CompilerParams(vmem_limit_bytes=8 * 2**20),
        name="sum_and_spread",
    )(arrived)


def exchanged(pieces, axis):
    return lax.all_to_all(pieces, axis, split_axis=0, concat_axis=0, tiled=True)


def gathered(lines, axis):
    return from_everyone(lines, axis).reshape(-1, lines.shape[-1])


def packed_body(cap, tokens, expert_ids, slot_ids, kept_mask, route_weights, out):
    width = tokens.shape[1]
    target = jnp.where(kept_mask[...] > 0, expert_ids[...] * cap + slot_ids[...], DROPPED)
    weight = route_weights[...]
    first = weight.astype(bf16)
    rest = weight - first.astype(f32)
    second = rest.astype(bf16)
    third = (rest - second.astype(f32)).astype(bf16)
    digits = [(target // RADIX).astype(f32), (target % RADIX).astype(f32)]
    parts = digits + [first.astype(f32), second.astype(f32), third.astype(f32)]
    top = target.shape[0]
    spare = jnp.zeros((SIDE - len(parts) * top, target.shape[1]), f32)
    out[:, :width] = tokens[...]
    out[:, width:] = jnp.concatenate(parts + [spare], 0).T.astype(bf16)


def packed(tokens, cap, *routing):
    count, width = tokens.shape
    return pl.pallas_call(
        lambda *refs: packed_body(cap, *refs),
        out_shape=jax.ShapeDtypeStruct((count, width + SIDE), bf16),
        cost_estimate=cost(1e6, 6e5),
        name="packed",
    )(tokens, *(array.T for array in routing))


def want_slots(shape, dim, base, block_of):
    slot = lax.broadcasted_iota(jnp.int32, shape, dim)
    place, source = slot & 7, (slot >> 3) & 1
    return (base + block_of(slot >> 4) * 8 + place).astype(f32) + SHIFT * source.astype(f32)


def keys_of(routes, top, dim):
    for k in range(top):
        take = (lambda n: routes[n : n + 1, :]) if dim == 1 else (lambda n: routes[:, n : n + 1])
        key = take(k) * RADIX + take(top + k)
        token = lax.broadcasted_iota(jnp.int32, key.shape, dim)
        half = routes.shape[dim] // PAIR
        yield k, key + SHIFT * (token // half).astype(f32)


def pick_body(top, scaled, base_ref, routes_ref, rows_ref, out_ref):
    slots, width = rows_ref.shape[0] // PAIR, rows_ref.shape[1]
    routes = routes_ref[...].astype(f32).T
    want = (lax.broadcasted_iota(jnp.int32, (slots, slots), 0) + base_ref[0]).astype(f32)
    devices, experts, places = out_ref.shape[:3]
    blocks = []
    for source in range(PAIR):
        part = slice(source * slots, (source + 1) * slots)
        chosen = jnp.zeros((slots, slots), f32)
        scale = jnp.zeros((slots, slots), f32)
        for k in range(top):
            own = [routes[n * top + k : n * top + k + 1, part] for n in range(5)]
            hit = own[0] * RADIX + own[1] == want
            chosen = jnp.where(hit, 1.0, chosen)
            if scaled:
                scale = jnp.where(hit, own[2] + own[3] + own[4], scale)
        picked = dot(chosen.astype(bf16), rows_ref[part])
        if scaled:
            picked = picked * jnp.sum(scale, axis=1, keepdims=True)
        blocks.append(picked.reshape(devices, experts, places // PAIR, width))
    out_ref[...] = jnp.concatenate(blocks, 2).astype(bf16)


def pick(base, routed, rows, width, top, scaled, devices, experts, cap):
    slots = devices * experts * cap * PAIR
    steps = rows.shape[0] // slots
    return pl.pallas_call(
        lambda *refs: pick_body(top, scaled, *refs),
        out_shape=jax.ShapeDtypeStruct((devices, experts, steps * PAIR * cap, width), bf16),
        grid_spec=pltpu.PrefetchScalarGridSpec(
            num_scalar_prefetch=1,
            grid=(steps,),
            in_specs=[
                pl.BlockSpec((slots, SIDE), lambda i, b: (i, width // SIDE)),
                pl.BlockSpec((slots, width), lambda i, b: (i, 0)),
            ],
            out_specs=pl.BlockSpec(
                (devices, experts, PAIR * cap, width), lambda i, b: (0, 0, i, 0)
            ),
        ),
        cost_estimate=cost(2 * slots * slots * width * steps, 4 * slots * width * steps),
        name="pick_scaled" if scaled else "pick",
    )(base, routed, rows)


def give_back_body(top, base_ref, routes_ref, *refs):
    *row_refs, out_ref = refs
    slots = out_ref.shape[0]
    devices = len(row_refs)
    routes = routes_ref[...].astype(f32)
    here = base_ref[1]

    def block_of(block):
        return ((here - (block >> 1)) & (devices - 1)) * 2 + (block & 1)

    want = want_slots((slots, slots), 1, base_ref[0], block_of)
    chosen = jnp.zeros((slots, slots), f32)
    for _, key in keys_of(routes, top, 0):
        chosen = jnp.where(key == want, 1.0, chosen)
    width = out_ref.shape[1]
    rows = jnp.concatenate([r[...].reshape(slots // devices, width) for r in row_refs], 0)
    out_ref[...] = dot(chosen.astype(bf16), rows).astype(bf16)


def give_back(base, routed, pieces, top, cap):
    experts, all_rows, width = pieces[0].shape
    steps = all_rows // (PAIR * cap)
    slots = len(pieces) * experts * PAIR * cap
    return pl.pallas_call(
        lambda *refs: give_back_body(top, *refs),
        out_shape=jax.ShapeDtypeStruct((steps * slots, width), bf16),
        grid_spec=pltpu.PrefetchScalarGridSpec(
            num_scalar_prefetch=1,
            grid=(steps,),
            in_specs=[pl.BlockSpec((slots, SIDE), lambda i, b: (i, width // SIDE))]
            + [pl.BlockSpec((experts, PAIR * cap, width), lambda i, b: (0, i, 0))] * len(pieces),
            out_specs=pl.BlockSpec((slots, width), lambda i, b: (i, 0)),
        ),
        cost_estimate=cost(2 * slots * slots * width * steps, 4 * slots * width * steps),
        name="give_back",
    )(base, routed, *pieces)


def flat(ref):
    value = ref[...]
    return value.reshape(-1, value.shape[-1])


def forward_body(x, gate_w, up_w, proj, act, slope_up, hidden, x_proj):
    rows = flat(x)
    gate, upper = dot(rows, gate_w[0]), dot(rows, up_w[0])
    sigma = jax.nn.sigmoid(gate)
    activated = gate * sigma
    act[0] = activated
    slope_up[0] = upper * (sigma * (1.0 + gate * (1.0 - sigma)))
    hidden[0] = (activated * upper).astype(bf16)
    x_proj[0] = dot(rows, proj[...]).astype(bf16)


def forward(x, gate_w, up_w, proj):
    plane, experts, depth, width = x.shape
    hid, rank = gate_w.shape[2], proj.shape[1]
    rows = plane * depth
    part = plane // 2
    weight = pl.BlockSpec((1, width, hid), lambda j, s: (j, 0, 0))
    out = lambda n: pl.BlockSpec((1, part * depth, n), lambda j, s: (j, s, 0))
    shape = lambda n, t: jax.ShapeDtypeStruct((experts, rows, n), t)
    return pl.pallas_call(
        forward_body,
        out_shape=(shape(hid, f32), shape(hid, f32), shape(hid, bf16), shape(rank, bf16)),
        grid=(experts, 2),
        in_specs=[pl.BlockSpec((part, 1, depth, width), lambda j, s: (s, j, 0, 0))]
        + [weight] * 2
        + [pl.BlockSpec((width, rank), lambda j, s: (0, 0))],
        out_specs=(out(hid), out(hid), out(hid), out(rank)),
        cost_estimate=cost(2 * experts * rows * width * (2 * hid + rank), 16e6),
        name="forward",
    )(x, gate_w, up_w, proj)


def backward_body(dy, down_w, proj, act, slope_up, hidden, x_proj, gate_grad, up_grad, grads):
    rows = flat(dy)
    hidden_grad = dot(rows, down_w[0], ((1,), (1,)))
    dy_proj = dot(rows, proj[...]).astype(bf16)
    of_up = (hidden_grad * act[0]).astype(bf16)
    of_gate = (hidden_grad * slope_up[0]).astype(bf16)
    up_grad[0] = of_up
    gate_grad[0] = of_gate
    over = ((0,), (0,))
    grads[0, 0] = dot(of_gate, x_proj[0], over).astype(bf16)
    grads[0, 1] = dot(of_up, x_proj[0], over).astype(bf16)
    grads[0, 2] = dot(hidden[0], dy_proj, over).astype(bf16)


def backward(dy, down_w, proj, act, slope_up, hidden, x_proj):
    plane, experts, depth, width = dy.shape
    hid, rank = down_w.shape[1], proj.shape[1]
    rows = plane * depth
    mat = lambda n: pl.BlockSpec((1, rows, n), lambda j: (j, 0, 0))
    shape = jax.ShapeDtypeStruct((experts, rows, hid), bf16)
    return pl.pallas_call(
        backward_body,
        out_shape=(shape, shape, jax.ShapeDtypeStruct((experts, 3, hid, rank), bf16)),
        grid=(experts,),
        in_specs=[
            pl.BlockSpec((plane, 1, depth, width), lambda j: (0, j, 0, 0)),
            pl.BlockSpec((1, hid, width), lambda j: (j, 0, 0)),
            pl.BlockSpec((width, rank), lambda j: (0, 0)),
            mat(hid), mat(hid), mat(hid), mat(rank),
        ],
        out_specs=(mat(hid), mat(hid), pl.BlockSpec((1, 3, hid, rank), lambda j: (j, 0, 0, 0))),
        cost_estimate=cost(2 * experts * rows * (width * (hid + rank) + 3 * hid * rank), 16e6),
        name="backward",
    )(dy, down_w, proj, act, slope_up, hidden, x_proj)


def row_grads_body(gate_grad, up_grad, gate_w, up_w, out):
    over = ((1,), (1,))
    value = dot(gate_grad[0], gate_w[0], over) + dot(up_grad[0], up_w[0], over)
    out[...] = value.astype(bf16).reshape(out.shape)


def row_grads_of(gate_grad, up_grad, gate_w, up_w, plane):
    experts, rows, hid = gate_grad.shape
    width = gate_w.shape[1]
    depth, part = rows // plane, plane // 2
    mat = pl.BlockSpec((1, rows // 2, hid), lambda j, s: (j, s, 0))
    weight = pl.BlockSpec((1, width, hid), lambda j, s: (j, 0, 0))
    return pl.pallas_call(
        row_grads_body,
        out_shape=jax.ShapeDtypeStruct((plane, experts, depth, width), bf16),
        grid=(experts, 2),
        in_specs=[mat, mat, weight, weight],
        out_specs=pl.BlockSpec((part, 1, depth, width), lambda j, s: (s, j, 0, 0)),
        cost_estimate=cost(4 * experts * rows * width * hid, 12e6),
        name="row_grads",
    )(gate_grad, up_grad, gate_w, up_w)


def weight_grads_body(x, dy, gate_grad, up_grad, hidden, out):
    hid = hidden.shape[-1]
    over = ((0,), (0,))
    out[:, 0:hid] = dot(flat(x), gate_grad[0], over).astype(bf16)
    out[:, hid : 2 * hid] = dot(flat(x), up_grad[0], over).astype(bf16)
    out[:, 2 * hid : 3 * hid] = dot(flat(dy), hidden[0], over).astype(bf16)


def weight_grads(x, dy, gate_grad, up_grad, hidden):
    plane, experts, depth, width = x.shape
    rows, hid = plane * depth, hidden.shape[2]
    part = width // 2
    row_spec = pl.BlockSpec((plane, 1, depth, part), lambda j, n: (0, j, 0, n))
    mat = pl.BlockSpec((1, rows, hid), lambda j, n: (j, 0, 0))
    return pl.pallas_call(
        weight_grads_body,
        out_shape=jax.ShapeDtypeStruct((width, 3 * hid * experts), bf16),
        grid=(experts, 2),
        in_specs=[row_spec] * 2 + [mat] * 3,
        out_specs=pl.BlockSpec((part, 3 * hid), lambda j, n: (n, j)),
        cost_estimate=cost(6 * experts * rows * width * hid, 24e6),
        compiler_params=pltpu.CompilerParams(vmem_limit_bytes=36 * 2**20),
        name="weight_grads",
    )(x, dy, gate_grad, up_grad, hidden)


def power_body(weights, grads, out):
    out[...] = dot(weights[...], grads[...]).astype(bf16)


def power_of(weights, grads):
    width, depth = weights.shape
    rank = grads.shape[1]
    part = width // 8
    return pl.pallas_call(
        power_body,
        out_shape=jax.ShapeDtypeStruct((width, rank), bf16),
        grid=(8,),
        in_specs=[
            pl.BlockSpec((part, depth), lambda i: (i, 0)),
            pl.BlockSpec((depth, rank), lambda i: (0, 0)),
        ],
        out_specs=pl.BlockSpec((part, rank), lambda i: (i, 0)),
        cost_estimate=cost(2 * width * depth * rank, 12e6),
        compiler_params=pltpu.CompilerParams(vmem_limit_bytes=58 * 2**20),
        name="power",
    )(weights, grads)


def inverse_factor(square):
    size = square.shape[0]
    row = lax.broadcasted_iota(jnp.int32, (size, 2 * size), 0)
    lane = lax.broadcasted_iota(jnp.int32, (size, 2 * size), 1)
    work = jnp.concatenate([square, jnp.zeros_like(square)], 1)
    work = jnp.where(lane == row + size, 1.0, work)
    groups = [work[g : g + 8] for g in range(0, size, 8)]
    scales = [jnp.zeros((8, 2 * size), f32) for _ in groups]
    inner = lax.broadcasted_iota(jnp.int32, (8, 2 * size), 0)
    for j in range(0, size, 2):
        g, at = divmod(j, 8)
        spread = [jnp.broadcast_to(w[:, j : j + 1], (8, 2 * size)) for w in groups[g:]]
        beside = [jnp.broadcast_to(w[:, j + 1 : j + 2], (8, 2 * size)) for w in groups[g:]]
        pivot, under = spread[0][at : at + 1], spread[0][at + 1 : at + 2]
        share = 1.0 / pivot
        line = groups[g][at : at + 1] * share
        across = beside[0][at : at + 1] * share
        next_pivot = beside[0][at + 1 : at + 2] - under * across
        next_line = (groups[g][at + 1 : at + 2] - under * line) / next_pivot
        scale = jnp.where(inner == at + 1, lax.rsqrt(next_pivot), scales[g])
        scales[g] = jnp.where(inner == at, lax.rsqrt(pivot), scale)
        for n in range(g, len(groups)):
            first, second = spread[n - g], beside[n - g] - spread[n - g] * across
            if n == g:
                first = jnp.where(inner > at, first, 0.0)
                second = jnp.where(inner > at + 1, second, 0.0)
            groups[n] = groups[n] - first * line - second * next_line
    return jnp.concatenate([w * s for w, s in zip(groups, scales)], 0)


def new_basis_body(scale, index_ref, power, own, out, gram, side, solved):
    size = power.shape[1]
    exact = lax.Precision.HIGHEST
    over = ((0,), (0,))
    gram[...] = dot(power[...], power[...], over)
    panel = own[...].astype(f32)
    spare = jnp.zeros((SIDE - panel.shape[0], size), f32)
    side[...] = jnp.concatenate([panel, spare], 0).T

    def step(k, _):
        head = gram[0:BLOCK]
        factor = inverse_factor(head[:, 0:BLOCK])
        none = jnp.zeros_like(head)
        lines = dot(factor, jnp.concatenate([none, head], 0), precision=exact)
        head = side[0:BLOCK]
        answer = dot(factor, jnp.concatenate([jnp.zeros_like(head), head], 0), precision=exact)
        solved[pl.ds(pl.multiple_of(k * BLOCK, BLOCK), BLOCK)] = answer
        lower = lines[:, BLOCK:]
        rest = gram[BLOCK:] - dot(lower, lines, over, exact)
        rest = jnp.concatenate([rest[:, BLOCK:], jnp.zeros((size - BLOCK, BLOCK), f32)], 1)
        gram[0 : size - BLOCK] = rest
        side[0 : size - BLOCK] = side[BLOCK:] - dot(lower, answer, over, exact)
        return 0

    lax.fori_loop(0, size // BLOCK, step, 0)
    out[...] = scale * solved[...].T[: out.shape[0]]


def new_basis_of(power, index, panel_rows):
    width, rank = power.shape
    return pl.pallas_call(
        lambda *refs: new_basis_body(math.sqrt(width), *refs),
        out_shape=jax.ShapeDtypeStruct((panel_rows, rank), f32),
        grid_spec=pltpu.PrefetchScalarGridSpec(
            num_scalar_prefetch=1,
            grid=(1,),
            in_specs=[
                pl.BlockSpec((width, rank), lambda i, n: (0, 0)),
                pl.BlockSpec((panel_rows, rank), lambda i, n: (n[0], 0)),
            ],
            out_specs=pl.BlockSpec((panel_rows, rank), lambda i, n: (0, 0)),
            scratch_shapes=[
                pltpu.VMEM((rank, rank), f32),
                pltpu.VMEM((rank, SIDE), f32),
                pltpu.VMEM((rank, SIDE), f32),
            ],
        ),
        cost_estimate=cost(3e10, 2e6),
        compiler_params=pltpu.CompilerParams(vmem_limit_bytes=24 * 2**20),
        name="new_basis",
    )(index, power, power)


def layer(
    tokens,
    cotangent,
    route_weights,
    expert_ids,
    slot_ids,
    kept_mask,
    gate_weight,
    up_weight,
    down_weight,
    projector_basis,
):
    tok_count, model_width = tokens.shape
    top = expert_ids.shape[1]
    experts = gate_weight.shape[0]
    group_count = lax.axis_size(EXPERT)
    plane = lax.axis_size(PLANE)
    cap = tok_count * top // (experts * group_count)
    here = lax.axis_index(PLANE)
    base = jnp.stack([lax.axis_index(Z) * (plane * experts * cap), here]).astype(jnp.int32)

    def along_z(value):
        return lax.all_gather(value, Z, axis=0, tiled=True)

    def after(value, *earlier):
        return lax.optimization_barrier((value, *earlier))

    first_rows = packed(tokens, cap, expert_ids, slot_ids, kept_mask, route_weights)

    panel_rows, rank = projector_basis.shape
    replicas = lax.axis_size(Y)
    share = panel_rows // replicas
    projector = (projector_basis * (1.0 / math.sqrt(model_width))).astype(bf16)
    projector = lax.dynamic_slice_in_dim(projector, lax.axis_index(Y) * share, share, 0)
    projector, first_rows = after(projector, first_rows)
    pieces = from_everyone(gathered(projector, (Z, X)), (C, Y))
    pieces = pieces.reshape(lax.axis_size(C), replicas, -1, share, rank)
    projector = pieces.transpose(2, 0, 1, 3, 4).reshape(model_width, rank)

    x_all = along_z(first_rows)
    dy_in, x_all, projector = after(cotangent, x_all, projector)
    dy_all = along_z(dy_in)

    def sent(rows, scaled):
        picked = pick(base, x_all, rows, model_width, top, scaled, plane, experts, cap)
        return lax.all_to_all(picked, PLANE, split_axis=0, concat_axis=0, tiled=True)

    x, dy = sent(x_all, False), sent(dy_all, True)
    act, slope_up, hidden, x_proj = forward(x, gate_weight, up_weight, projector)
    gate_grad, up_grad, partial = backward(
        dy, down_weight, projector, act, slope_up, hidden, x_proj
    )

    arrived = exchanged(partial.reshape(replicas, -1, partial.shape[-1]), Y)
    spread = sum_and_spread(arrived, 3)
    grads_low = exchanged(spread, Y)
    projected_grads = grads_low.astype(f32).reshape(partial.shape)
    grads_low = grads_low.reshape(-1, partial.shape[-1])

    rows = row_grads_of(gate_grad, up_grad, gate_weight, up_weight, plane)
    returned = []
    for d in range(plane):
        piece = lax.dynamic_index_in_dim(rows, (here + d) % plane, 0, keepdims=False)
        if d:
            piece = lax.ppermute(piece, PLANE, [(i, (i + d) % plane) for i in range(plane)])
        returned.append(piece)

    late_gate_grad, _ = after(gate_grad, spread)
    own_weight_grads = weight_grads(x, dy, late_gate_grad, up_grad, hidden)
    near, far = (C, Y), (Z, X)
    power = power_of(own_weight_grads, grads_low)
    late_base, power = after(base, power)
    power = sent_and_summed(power, near)
    power = exchanged(power.reshape(lax.axis_size(far), -1, power.shape[-1]), far)
    power = exchanged(sum_and_spread(power, 1), far).reshape(-1, power.shape[-1])
    power = gathered(power, near)

    token_parts = give_back(late_base, x_all, returned, top, cap)
    token_grads = lax.psum_scatter(token_parts, Z, scatter_dimension=0, tiled=True)

    index = lax.axis_index(EXPERT).astype(jnp.int32).reshape(1)
    new_basis = new_basis_of(power, index, model_width // group_count)
    return (token_grads, projected_grads, new_basis)


def solution(mesh):
    finer = Mesh(mesh.devices.reshape(8, 4, 2, mesh.shape["replica"]), EXPERT_REPLICA)
    rows = P(EXPERT_REPLICA, None)
    placed = (rows,) * 6 + (P(EXPERT, None, None),) * 3 + (P(EXPERT, None),)
    return jax.shard_map(
        layer,
        mesh=finer,
        in_specs=placed,
        out_specs=(rows, P(EXPERT, None, None, None), P(EXPERT, None)),
        check_vma=False,
    )
```

```python
import math

import jax
import jax.numpy as jnp
from jax import lax
from jax.experimental import pallas as pl
from jax.experimental.pallas import tpu as pltpu
from jax.sharding import Mesh
from jax.sharding import PartitionSpec as P

Z, X, C, Y = "expert_0", "expert_1", "expert_2", "replica"
EXPERT = (Z, X, C)
EXPERT_REPLICA = (Z, X, C, Y)
PLANE = (X, C)
PAIR = 2
RADIX = 256
DROPPED = 255 * RADIX
SHIFT = float(1 << 17)
SIDE = 128
BLOCK = 64


f32, bf16 = jnp.float32, jnp.bfloat16


def dot(a, b, over=((1,), (0,)), precision=None):
    return lax.dot_general(a, b, (over, ((), ())), precision=precision, preferred_element_type=f32)


def cost(flops, nbytes):
    return pl.CostEstimate(flops=int(flops), bytes_accessed=int(nbytes), transcendentals=0)


def from_everyone(array, axis):
    copies = jnp.broadcast_to(array, (lax.axis_size(axis), *array.shape))
    return lax.all_to_all(copies, axis, split_axis=0, concat_axis=0, tiled=True)


def sent_and_summed(lines, axis):
    devices = lax.axis_size(axis)
    pieces = lines.reshape(devices, -1, lines.shape[-1])
    arrived = lax.all_to_all(pieces, axis, split_axis=0, concat_axis=0, tiled=True)
    return arrived.astype(f32).sum(axis=0).astype(bf16)


def sum_and_spread_body(arrived, out):
    total = arrived[...].astype(f32).sum(axis=0).astype(bf16)
    out[...] = jnp.broadcast_to(total[None], out.shape)


def sum_and_spread(arrived, steps):
    devices, lines, width = arrived.shape
    spec = pl.BlockSpec((devices, lines // steps, width), lambda i: (0, i, 0))
    return pl.pallas_call(
        sum_and_spread_body,
        out_shape=jax.ShapeDtypeStruct(arrived.shape, bf16),
        grid=(steps,),
        in_specs=[spec],
        out_specs=spec,
        cost_estimate=cost(arrived.size, 4 * arrived.size),
        compiler_params=pltpu.CompilerParams(vmem_limit_bytes=8 * 2**20),
        name="sum_and_spread",
    )(arrived)


def exchanged(pieces, axis):
    return lax.all_to_all(pieces, axis, split_axis=0, concat_axis=0, tiled=True)


def gathered(lines, axis):
    return from_everyone(lines, axis).reshape(-1, lines.shape[-1])


def packed_body(cap, tokens, expert_ids, slot_ids, kept_mask, route_weights, out):
    width = tokens.shape[1]
    target = jnp.where(kept_mask[...] > 0, expert_ids[...] * cap + slot_ids[...], DROPPED)
    weight = route_weights[...]
    first = weight.astype(bf16)
    rest = weight - first.astype(f32)
    second = rest.astype(bf16)
    third = (rest - second.astype(f32)).astype(bf16)
    digits = [(target // RADIX).astype(f32), (target % RADIX).astype(f32)]
    parts = digits + [first.astype(f32), second.astype(f32), third.astype(f32)]
    top = target.shape[0]
    spare = jnp.zeros((SIDE - len(parts) * top, target.shape[1]), f32)
    out[:, :width] = tokens[...]
    out[:, width:] = jnp.concatenate(parts + [spare], 0).T.astype(bf16)


def packed(tokens, cap, *routing):
    count, width = tokens.shape
    return pl.pallas_call(
        lambda *refs: packed_body(cap, *refs),
        out_shape=jax.ShapeDtypeStruct((count, width + SIDE), bf16),
        cost_estimate=cost(1e6, 6e5),
        name="packed",
    )(tokens, *(array.T for array in routing))


def want_slots(shape, dim, base, block_of):
    slot = lax.broadcasted_iota(jnp.int32, shape, dim)
    place, source = slot & 7, (slot >> 3) & 1
    return (base + block_of(slot >> 4) * 8 + place).astype(f32) + SHIFT * source.astype(f32)


def keys_of(routes, top, dim):
    for k in range(top):
        take = (lambda n: routes[n : n + 1, :]) if dim == 1 else (lambda n: routes[:, n : n + 1])
        key = take(k) * RADIX + take(top + k)
        token = lax.broadcasted_iota(jnp.int32, key.shape, dim)
        half = routes.shape[dim] // PAIR
        yield k, key + SHIFT * (token // half).astype(f32)


def pick_body(top, scaled, base_ref, routes_ref, rows_ref, out_ref):
    slots, width = rows_ref.shape[0] // PAIR, rows_ref.shape[1]
    routes = routes_ref[...].astype(f32).T
    want = (lax.broadcasted_iota(jnp.int32, (slots, slots), 0) + base_ref[0]).astype(f32)
    devices, experts, places = out_ref.shape[:3]
    blocks = []
    for source in range(PAIR):
        part = slice(source * slots, (source + 1) * slots)
        chosen = jnp.zeros((slots, slots), f32)
        scale = jnp.zeros((slots, slots), f32)
        for k in range(top):
            own = [routes[n * top + k : n * top + k + 1, part] for n in range(5)]
            hit = own[0] * RADIX + own[1] == want
            chosen = jnp.where(hit, 1.0, chosen)
            if scaled:
                scale = jnp.where(hit, own[2] + own[3] + own[4], scale)
        picked = dot(chosen.astype(bf16), rows_ref[part])
        if scaled:
            picked = picked * jnp.sum(scale, axis=1, keepdims=True)
        blocks.append(picked.reshape(devices, experts, places // PAIR, width))
    out_ref[...] = jnp.concatenate(blocks, 2).astype(bf16)


def pick(base, routed, rows, width, top, scaled, devices, experts, cap):
    slots = devices * experts * cap * PAIR
    steps = rows.shape[0] // slots
    return pl.pallas_call(
        lambda *refs: pick_body(top, scaled, *refs),
        out_shape=jax.ShapeDtypeStruct((devices, experts, steps * PAIR * cap, width), bf16),
        grid_spec=pltpu.PrefetchScalarGridSpec(
            num_scalar_prefetch=1,
            grid=(steps,),
            in_specs=[
                pl.BlockSpec((slots, SIDE), lambda i, b: (i, width // SIDE)),
                pl.BlockSpec((slots, width), lambda i, b: (i, 0)),
            ],
            out_specs=pl.BlockSpec(
                (devices, experts, PAIR * cap, width), lambda i, b: (0, 0, i, 0)
            ),
        ),
        cost_estimate=cost(2 * slots * slots * width * steps, 4 * slots * width * steps),
        name="pick_scaled" if scaled else "pick",
    )(base, routed, rows)


def give_back_body(top, base_ref, routes_ref, *refs):
    *row_refs, out_ref = refs
    slots = out_ref.shape[0]
    devices = len(row_refs)
    routes = routes_ref[...].astype(f32)
    here = base_ref[1]

    def block_of(block):
        return ((here - (block >> 1)) & (devices - 1)) * 2 + (block & 1)

    want = want_slots((slots, slots), 1, base_ref[0], block_of)
    chosen = jnp.zeros((slots, slots), f32)
    for _, key in keys_of(routes, top, 0):
        chosen = jnp.where(key == want, 1.0, chosen)
    width = out_ref.shape[1]
    rows = jnp.concatenate([r[...].reshape(slots // devices, width) for r in row_refs], 0)
    out_ref[...] = dot(chosen.astype(bf16), rows).astype(bf16)


def give_back(base, routed, pieces, top, cap):
    experts, all_rows, width = pieces[0].shape
    steps = all_rows // (PAIR * cap)
    slots = len(pieces) * experts * PAIR * cap
    return pl.pallas_call(
        lambda *refs: give_back_body(top, *refs),
        out_shape=jax.ShapeDtypeStruct((steps * slots, width), bf16),
        grid_spec=pltpu.PrefetchScalarGridSpec(
            num_scalar_prefetch=1,
            grid=(steps,),
            in_specs=[pl.BlockSpec((slots, SIDE), lambda i, b: (i, width // SIDE))]
            + [pl.BlockSpec((experts, PAIR * cap, width), lambda i, b: (0, i, 0))] * len(pieces),
            out_specs=pl.BlockSpec((slots, width), lambda i, b: (i, 0)),
        ),
        cost_estimate=cost(2 * slots * slots * width * steps, 4 * slots * width * steps),
        name="give_back",
    )(base, routed, *pieces)


def flat(ref):
    value = ref[...]
    return value.reshape(-1, value.shape[-1])


def forward_body(x, gate_w, up_w, proj, act, slope_up, hidden, x_proj):
    rows = flat(x)
    gate, upper = dot(rows, gate_w[0]), dot(rows, up_w[0])
    sigma = jax.nn.sigmoid(gate)
    activated = gate * sigma
    act[0] = activated
    slope_up[0] = upper * (sigma * (1.0 + gate * (1.0 - sigma)))
    hidden[0] = (activated * upper).astype(bf16)
    x_proj[0] = dot(rows, proj[...]).astype(bf16)


def forward(x, gate_w, up_w, proj):
    plane, experts, depth, width = x.shape
    hid, rank = gate_w.shape[2], proj.shape[1]
    rows = plane * depth
    part = plane // 2
    weight = pl.BlockSpec((1, width, hid), lambda j, s: (j, 0, 0))
    out = lambda n: pl.BlockSpec((1, part * depth, n), lambda j, s: (j, s, 0))
    shape = lambda n, t: jax.ShapeDtypeStruct((experts, rows, n), t)
    return pl.pallas_call(
        forward_body,
        out_shape=(shape(hid, f32), shape(hid, f32), shape(hid, bf16), shape(rank, bf16)),
        grid=(experts, 2),
        in_specs=[pl.BlockSpec((part, 1, depth, width), lambda j, s: (s, j, 0, 0))]
        + [weight] * 2
        + [pl.BlockSpec((width, rank), lambda j, s: (0, 0))],
        out_specs=(out(hid), out(hid), out(hid), out(rank)),
        cost_estimate=cost(2 * experts * rows * width * (2 * hid + rank), 16e6),
        name="forward",
    )(x, gate_w, up_w, proj)


def backward_body(dy, down_w, proj, act, slope_up, hidden, x_proj, gate_grad, up_grad, grads):
    rows = flat(dy)
    hidden_grad = dot(rows, down_w[0], ((1,), (1,)))
    dy_proj = dot(rows, proj[...]).astype(bf16)
    of_up = (hidden_grad * act[0]).astype(bf16)
    of_gate = (hidden_grad * slope_up[0]).astype(bf16)
    up_grad[0] = of_up
    gate_grad[0] = of_gate
    over = ((0,), (0,))
    grads[0, 0] = dot(of_gate, x_proj[0], over).astype(bf16)
    grads[0, 1] = dot(of_up, x_proj[0], over).astype(bf16)
    grads[0, 2] = dot(hidden[0], dy_proj, over).astype(bf16)


def backward(dy, down_w, proj, act, slope_up, hidden, x_proj):
    plane, experts, depth, width = dy.shape
    hid, rank = down_w.shape[1], proj.shape[1]
    rows = plane * depth
    mat = lambda n: pl.BlockSpec((1, rows, n), lambda j: (j, 0, 0))
    shape = jax.ShapeDtypeStruct((experts, rows, hid), bf16)
    return pl.pallas_call(
        backward_body,
        out_shape=(shape, shape, jax.ShapeDtypeStruct((experts, 3, hid, rank), bf16)),
        grid=(experts,),
        in_specs=[
            pl.BlockSpec((plane, 1, depth, width), lambda j: (0, j, 0, 0)),
            pl.BlockSpec((1, hid, width), lambda j: (j, 0, 0)),
            pl.BlockSpec((width, rank), lambda j: (0, 0)),
            mat(hid), mat(hid), mat(hid), mat(rank),
        ],
        out_specs=(mat(hid), mat(hid), pl.BlockSpec((1, 3, hid, rank), lambda j: (j, 0, 0, 0))),
        cost_estimate=cost(2 * experts * rows * (width * (hid + rank) + 3 * hid * rank), 16e6),
        name="backward",
    )(dy, down_w, proj, act, slope_up, hidden, x_proj)


def row_grads_body(gate_grad, up_grad, gate_w, up_w, out):
    over = ((1,), (1,))
    value = dot(gate_grad[0], gate_w[0], over) + dot(up_grad[0], up_w[0], over)
    out[...] = value.astype(bf16).reshape(out.shape)


def row_grads_of(gate_grad, up_grad, gate_w, up_w, plane):
    experts, rows, hid = gate_grad.shape
    width = gate_w.shape[1]
    depth, part = rows // plane, plane // 2
    mat = pl.BlockSpec((1, rows // 2, hid), lambda j, s: (j, s, 0))
    weight = pl.BlockSpec((1, width, hid), lambda j, s: (j, 0, 0))
    return pl.pallas_call(
        row_grads_body,
        out_shape=jax.ShapeDtypeStruct((plane, experts, depth, width), bf16),
        grid=(experts, 2),
        in_specs=[mat, mat, weight, weight],
        out_specs=pl.BlockSpec((part, 1, depth, width), lambda j, s: (s, j, 0, 0)),
        cost_estimate=cost(4 * experts * rows * width * hid, 12e6),
        name="row_grads",
    )(gate_grad, up_grad, gate_w, up_w)


def weight_grads_body(x, dy, gate_grad, up_grad, hidden, out):
    hid = hidden.shape[-1]
    over = ((0,), (0,))
    out[:, 0:hid] = dot(flat(x), gate_grad[0], over).astype(bf16)
    out[:, hid : 2 * hid] = dot(flat(x), up_grad[0], over).astype(bf16)
    out[:, 2 * hid : 3 * hid] = dot(flat(dy), hidden[0], over).astype(bf16)


def weight_grads(x, dy, gate_grad, up_grad, hidden):
    plane, experts, depth, width = x.shape
    rows, hid = plane * depth, hidden.shape[2]
    part = width // 2
    row_spec = pl.BlockSpec((plane, 1, depth, part), lambda j, n: (0, j, 0, n))
    mat = pl.BlockSpec((1, rows, hid), lambda j, n: (j, 0, 0))
    return pl.pallas_call(
        weight_grads_body,
        out_shape=jax.ShapeDtypeStruct((width, 3 * hid * experts), bf16),
        grid=(experts, 2),
        in_specs=[row_spec] * 2 + [mat] * 3,
        out_specs=pl.BlockSpec((part, 3 * hid), lambda j, n: (n, j)),
        cost_estimate=cost(6 * experts * rows * width * hid, 24e6),
        compiler_params=pltpu.CompilerParams(vmem_limit_bytes=36 * 2**20),
        name="weight_grads",
    )(x, dy, gate_grad, up_grad, hidden)


def inverse_factor(square):
    size = square.shape[0]
    row = lax.broadcasted_iota(jnp.int32, (size, 2 * size), 0)
    lane = lax.broadcasted_iota(jnp.int32, (size, 2 * size), 1)
    work = jnp.concatenate([square, jnp.zeros_like(square)], 1)
    work = jnp.where(lane == row + size, 1.0, work)
    groups = [work[g : g + 8] for g in range(0, size, 8)]
    scales = [jnp.zeros((8, 2 * size), f32) for _ in groups]
    inner = lax.broadcasted_iota(jnp.int32, (8, 2 * size), 0)
    for j in range(0, size, 2):
        g, at = divmod(j, 8)
        spread = [jnp.broadcast_to(w[:, j : j + 1], (8, 2 * size)) for w in groups[g:]]
        beside = [jnp.broadcast_to(w[:, j + 1 : j + 2], (8, 2 * size)) for w in groups[g:]]
        pivot, under = spread[0][at : at + 1], spread[0][at + 1 : at + 2]
        share = 1.0 / pivot
        line = groups[g][at : at + 1] * share
        across = beside[0][at : at + 1] * share
        next_pivot = beside[0][at + 1 : at + 2] - under * across
        next_line = (groups[g][at + 1 : at + 2] - under * line) / next_pivot
        scale = jnp.where(inner == at + 1, lax.rsqrt(next_pivot), scales[g])
        scales[g] = jnp.where(inner == at, lax.rsqrt(pivot), scale)
        for n in range(g, len(groups)):
            first, second = spread[n - g], beside[n - g] - spread[n - g] * across
            if n == g:
                first = jnp.where(inner > at, first, 0.0)
                second = jnp.where(inner > at + 1, second, 0.0)
            groups[n] = groups[n] - first * line - second * next_line
    return jnp.concatenate([w * s for w, s in zip(groups, scales)], 0)


def new_basis_body(scale, index_ref, power, own, out, gram, side, solved):
    size = power.shape[1]
    exact = lax.Precision.HIGHEST
    over = ((0,), (0,))
    gram[...] = dot(power[...], power[...], over)
    panel = own[...].astype(f32)
    spare = jnp.zeros((SIDE - panel.shape[0], size), f32)
    side[...] = jnp.concatenate([panel, spare], 0).T

    def step(k, _):
        head = gram[0:BLOCK]
        factor = inverse_factor(head[:, 0:BLOCK])
        none = jnp.zeros_like(head)
        lines = dot(factor, jnp.concatenate([none, head], 0), precision=exact)
        head = side[0:BLOCK]
        answer = dot(factor, jnp.concatenate([jnp.zeros_like(head), head], 0), precision=exact)
        solved[pl.ds(pl.multiple_of(k * BLOCK, BLOCK), BLOCK)] = answer
        lower = lines[:, BLOCK:]
        rest = gram[BLOCK:] - dot(lower, lines, over, exact)
        rest = jnp.concatenate([rest[:, BLOCK:], jnp.zeros((size - BLOCK, BLOCK), f32)], 1)
        gram[0 : size - BLOCK] = rest
        side[0 : size - BLOCK] = side[BLOCK:] - dot(lower, answer, over, exact)
        return 0

    lax.fori_loop(0, size // BLOCK, step, 0)
    out[...] = scale * solved[...].T[: out.shape[0]]


def new_basis_of(power, index, panel_rows):
    width, rank = power.shape
    return pl.pallas_call(
        lambda *refs: new_basis_body(math.sqrt(width), *refs),
        out_shape=jax.ShapeDtypeStruct((panel_rows, rank), f32),
        grid_spec=pltpu.PrefetchScalarGridSpec(
            num_scalar_prefetch=1,
            grid=(1,),
            in_specs=[
                pl.BlockSpec((width, rank), lambda i, n: (0, 0)),
                pl.BlockSpec((panel_rows, rank), lambda i, n: (n[0], 0)),
            ],
            out_specs=pl.BlockSpec((panel_rows, rank), lambda i, n: (0, 0)),
            scratch_shapes=[
                pltpu.VMEM((rank, rank), f32),
                pltpu.VMEM((rank, SIDE), f32),
                pltpu.VMEM((rank, SIDE), f32),
            ],
        ),
        cost_estimate=cost(3e10, 2e6),
        compiler_params=pltpu.CompilerParams(vmem_limit_bytes=24 * 2**20),
        name="new_basis",
    )(index, power, power)


def layer(
    tokens,
    cotangent,
    route_weights,
    expert_ids,
    slot_ids,
    kept_mask,
    gate_weight,
    up_weight,
    down_weight,
    projector_basis,
):
    tok_count, model_width = tokens.shape
    top = expert_ids.shape[1]
    experts = gate_weight.shape[0]
    group_count = lax.axis_size(EXPERT)
    plane = lax.axis_size(PLANE)
    cap = tok_count * top // (experts * group_count)
    here = lax.axis_index(PLANE)
    base = jnp.stack([lax.axis_index(Z) * (plane * experts * cap), here]).astype(jnp.int32)

    def along_z(value):
        return lax.all_gather(value, Z, axis=0, tiled=True)

    def after(value, *earlier):
        return lax.optimization_barrier((value, *earlier))

    first_rows = packed(tokens, cap, expert_ids, slot_ids, kept_mask, route_weights)

    panel_rows, rank = projector_basis.shape
    replicas = lax.axis_size(Y)
    share = panel_rows // replicas
    projector = (projector_basis * (1.0 / math.sqrt(model_width))).astype(bf16)
    projector = lax.dynamic_slice_in_dim(projector, lax.axis_index(Y) * share, share, 0)
    projector, first_rows = after(projector, first_rows)
    pieces = from_everyone(gathered(projector, (Z, X)), (C, Y))
    pieces = pieces.reshape(lax.axis_size(C), replicas, -1, share, rank)
    projector = pieces.transpose(2, 0, 1, 3, 4).reshape(model_width, rank)

    x_all = along_z(first_rows)
    dy_in, x_all, projector = after(cotangent, x_all, projector)
    dy_all = along_z(dy_in)

    def sent(rows, scaled):
        picked = pick(base, x_all, rows, model_width, top, scaled, plane, experts, cap)
        return lax.all_to_all(picked, PLANE, split_axis=0, concat_axis=0, tiled=True)

    x, dy = sent(x_all, False), sent(dy_all, True)
    act, slope_up, hidden, x_proj = forward(x, gate_weight, up_weight, projector)
    gate_grad, up_grad, partial = backward(
        dy, down_weight, projector, act, slope_up, hidden, x_proj
    )

    arrived = exchanged(partial.reshape(replicas, -1, partial.shape[-1]), Y)
    rows = row_grads_of(gate_grad, up_grad, gate_weight, up_weight, plane)
    pieces = [
        lax.dynamic_index_in_dim(rows, (here + d) % plane, 0, keepdims=False) for d in range(plane)
    ]
    arrived, *pieces = after(arrived, *pieces)
    spread = sum_and_spread(arrived, 3)
    grads_low = exchanged(spread, Y)
    projected_grads = grads_low.astype(f32).reshape(partial.shape)
    grads_low = grads_low.reshape(-1, partial.shape[-1])

    returned = [pieces[0]]
    for d in range(1, plane):
        places = [(i, (i + d) % plane) for i in range(plane)]
        returned.append(lax.ppermute(pieces[d], PLANE, places))

    late_gate_grad, _ = after(gate_grad, spread)
    own_weight_grads = weight_grads(x, dy, late_gate_grad, up_grad, hidden)
    near, far = (C, Y), (Z, X)
    power = dot(own_weight_grads, grads_low).astype(bf16)
    power = sent_and_summed(power, near)
    late_base, power = after(base, power)
    power = exchanged(power.reshape(lax.axis_size(far), -1, power.shape[-1]), far)
    power = exchanged(sum_and_spread(power, 1), far).reshape(-1, power.shape[-1])
    power = gathered(power, near)

    token_parts = give_back(late_base, x_all, returned, top, cap)
    token_grads = lax.psum_scatter(token_parts, Z, scatter_dimension=0, tiled=True)

    index = lax.axis_index(EXPERT).astype(jnp.int32).reshape(1)
    new_basis = new_basis_of(power, index, model_width // group_count)
    return (token_grads, projected_grads, new_basis)


def solution(mesh):
    finer = Mesh(mesh.devices.reshape(8, 4, 2, mesh.shape["replica"]), EXPERT_REPLICA)
    rows = P(EXPERT_REPLICA, None)
    placed = (rows,) * 6 + (P(EXPERT, None, None),) * 3 + (P(EXPERT, None),)
    return jax.shard_map(
        layer,
        mesh=finer,
        in_specs=placed,
        out_specs=(rows, P(EXPERT, None, None, None), P(EXPERT, None)),
        check_vma=False,
    )
```
